8 devices in a mesh: data: 8 (over z, y, x, core).
Axes of the slice: x: 2, y: 2, z: 1, core: 2. Of those that a mesh axis runs over, the one named last changes fastest.
Arguments:
- act_in: bfloat16 [8192, 896], P('data')
- pre_act: bfloat16 [8192, 4864], P('data')
- grad_out: bfloat16 [8192, 4864], P('data')
- q_init: float32 [4864, 8], replicated
- err_mem: float32 [8, 896, 4864], P('data')
Outputs:
- output 1: float32 [896, 8], replicated
- output 2: float32 [4864, 8], replicated
- output 3: float32 [8, 896, 4864], P('data')
All inputs are finite; a program needn't handle non-finite values.
Results may differ from the reference program's by a relative error of at most 0.001.
Values sent between devices are 32-bit elements.
A program may use at most 1 GiB of HBM per device.

```python
import math
import jax
import jax.numpy as jnp
from jax import lax

GROUP_SIZE = 8
TOKENS = 1024
D_IN = 896
D_OUT = 4864
LOW_RANK = 8

MIX_RANK = 4 * LOW_RANK
COHERE = 2.0 * math.sqrt(max(1.0, D_IN / TOKENS))
DY_SCALE = math.sqrt(TOKENS)
ERR_SCALE = 0.6 * math.sqrt(1.0 + COHERE * COHERE)
EXACT_PREC = lax.Precision.HIGHEST


def setup_inputs(seed: int = 0) -> dict:
    key_list = jax.random.split(jax.random.key(seed), 7)
    all_rows = GROUP_SIZE * TOKENS
    act_f32 = jax.random.normal(key_list[0], (all_rows, D_IN), jnp.float32)
    mix_left = jax.random.normal(key_list[1], (D_IN, MIX_RANK), jnp.float32) * D_IN ** -0.5
    mix_right = jax.random.normal(key_list[2], (MIX_RANK, D_OUT), jnp.float32) * MIX_RANK ** -0.5
    signal = jnp.dot(jnp.dot(act_f32, mix_left), mix_right)
    noise_part = jax.random.normal(key_list[3], (all_rows, D_OUT), jnp.float32)
    grad_out = (COHERE * signal + noise_part) * DY_SCALE
    pre_act = jax.random.normal(key_list[4], (all_rows, D_OUT), jnp.float32)
    q_init = jax.random.normal(key_list[5], (D_OUT, LOW_RANK), jnp.float32) * D_OUT ** -0.5
    err_mem = jax.random.normal(key_list[6], (GROUP_SIZE, D_IN, D_OUT), jnp.float32) * ERR_SCALE
    return {'act_in': act_f32.astype(jnp.bfloat16), 'pre_act': pre_act.astype(jnp.bfloat16), 'grad_out': grad_out.astype(jnp.bfloat16), 'q_init': q_init, 'err_mem': err_mem}


def gelu_grad(pre_act, grad_out):
    z_f32 = pre_act.astype(jnp.float32)
    _, pullback = jax.vjp(jax.nn.gelu, z_f32)
    return pullback(grad_out.astype(jnp.float32))[0]


def orthonormalize(p_sum):
    def gs_step(col_idx, ortho_cols):
        column = lax.dynamic_slice_in_dim(p_sum, col_idx, 1, axis=1)
        proj_coef = jnp.dot(column.T, ortho_cols, precision=EXACT_PREC)
        residual = column - jnp.dot(ortho_cols, proj_coef.T, precision=EXACT_PREC)
        unit_col = residual / jnp.sqrt(jnp.sum(residual * residual))
        return lax.dynamic_update_slice_in_dim(ortho_cols, unit_col, col_idx, axis=1)
    return lax.fori_loop(0, p_sum.shape[1], gs_step, jnp.zeros_like(p_sum))


def reference(act_in, pre_act, grad_out, q_init, err_mem):
    act_dev = act_in.reshape(GROUP_SIZE, TOKENS, D_IN)
    pre_dev = pre_act.reshape(GROUP_SIZE, TOKENS, D_OUT)
    dy_dev = grad_out.reshape(GROUP_SIZE, TOKENS, D_OUT)

    def merged_grad(blk_tuple):
        act_blk, pre_blk, dy_blk, err_blk = blk_tuple
        grad_pre = gelu_grad(pre_blk, dy_blk).astype(jnp.bfloat16)
        grad_w = jnp.dot(act_blk.T, grad_pre, preferred_element_type=jnp.float32) / TOKENS
        return grad_w + err_blk

    merged = lax.map(merged_grad, (act_dev, pre_dev, dy_dev, err_mem))
    p_sum = jnp.einsum('gij,jr->ir', merged, q_init, precision=EXACT_PREC)
    p_factor = orthonormalize(p_sum)
    q_factor = jnp.einsum('gij,ir->jr', merged, p_factor, precision=EXACT_PREC) / GROUP_SIZE
    err_new = merged - jnp.dot(p_factor, q_factor.T, precision=EXACT_PREC)[None]
    return p_factor, q_factor, err_new
```

```python
import functools
import jax
import jax.numpy as jnp
from jax import lax
from jax.experimental import pallas as pl
from jax.experimental.pallas import tpu as pltpu
from jax.sharding import PartitionSpec as P

F32 = jnp.float32
BF16 = jnp.bfloat16
GROUP = 8
ROWS = 1024
D_IN = 896
D_OUT = 4864
RANK = 8
CHUNK = 256
N_CHUNK = D_OUT // CHUNK
HALF = D_OUT // 2
PIECES = ((0, 512), (512, 512), (1024, 512), (1536, 512), (2048, 384))
AHEAD = 6
MESH = pl.DeviceIdType.MESH
C0 = 0.7978845608028654
C1 = 0.044715


def split3(x):
    hi = x.astype(BF16)
    rest = x - hi.astype(F32)
    mid = rest.astype(BF16)
    low = (rest - mid.astype(F32)).astype(BF16)
    return hi, mid, low


def stack3(x):
    hi, mid, low = split3(x)
    return jnp.concatenate([hi.astype(F32), mid.astype(F32), low.astype(F32)], axis=0).astype(BF16)


def gelu_grad_times(z, dy):
    x = z.astype(F32)
    sq = x * x
    t = jnp.tanh(x * (C0 + (C0 * C1) * sq))
    s = 0.5 + 0.5 * t
    w = x * (2.0 * C0 + (6.0 * C0 * C1) * sq)
    return (s * (1.0 + (1.0 - s) * w) * dy.astype(F32)).astype(BF16)


def orthonormal_rows(p0):
    p0 = p0 / jnp.max(jnp.abs(p0), axis=1, keepdims=True)
    row = lax.broadcasted_iota(jnp.int32, (RANK, 1), 0)
    cur = p0
    for k in range(RANK):
        v = jnp.broadcast_to(cur[k:k + 1, :], cur.shape)
        inv = lax.rsqrt(jnp.sum(v * v, axis=1, keepdims=True))
        coef = jnp.sum(v * p0, axis=1, keepdims=True) * inv
        q = v * inv
        cur = jnp.where(row == k, q, cur - jnp.where(row > k, coef, 0.0) * q)
    return cur


def main_kernel(a_ref, z_hbm, dy_hbm, qt_ref, e_hbm, m_ref, pt_ref, qn_ref,
                z_v, dy_v, at_ref, g0_ref, g1_ref, pacc_ref, p_all, q_part, q_pair, q_all,
                sem_in, sem_ps, sem_pr, sem_q1, sem_q2s, sem_q2r, sem_q3):
    me = lax.axis_index('data')
    core = lax.rem(me, 2)
    chip = me // 2
    mate = me + 1 - 2 * core

    barrier = pltpu.get_barrier_semaphore()
    for d in range(1, GROUP):
        pl.semaphore_signal(barrier, inc=1, device_id=(lax.rem(me + d, GROUP),), device_id_type=MESH)

    def fetch(c, go):
        cols = pl.ds(pl.multiple_of(c * CHUNK, CHUNK), CHUNK)
        for k, (src, dst) in enumerate(((z_hbm, z_v), (dy_hbm, dy_v), (e_hbm, m_ref))):
            go(pltpu.make_async_copy(src.at[:, cols], dst.at[:, cols], sem_in.at[k, c]), k)

    def start(c):
        fetch(c, lambda cp, k: cp.start())

    def wait_zy(c):
        fetch(c, lambda cp, k: cp.wait() if k < 2 else None)

    def wait_e(c):
        fetch(c, lambda cp, k: cp.wait() if k == 2 else None)

    for c in range(AHEAD):
        start(c)
    at_ref[...] = a_ref[...].T
    pacc_ref[...] = jnp.zeros_like(pacc_ref)

    def make_g(c, g_ref):
        cols = pl.ds(pl.multiple_of(c * CHUNK, CHUNK), CHUNK)
        for r in range(0, ROWS, 64):
            rows = pl.ds(r, 64)
            g_ref[rows, :] = gelu_grad_times(z_v[rows, cols], dy_v[rows, cols])

    def use_g(c, g_ref):
        cols = pl.ds(pl.multiple_of(c * CHUNK, CHUNK), CHUNK)
        q3 = stack3(qt_ref[:, cols])
        m = jnp.dot(at_ref[...], g_ref[...], preferred_element_type=F32) * (1.0 / ROWS) + m_ref[:, cols]
        m_ref[:, cols] = m
        dims = (((1,), (1,)), ((), ()))
        acc = None
        for piece in split3(m):
            part = lax.dot_general(q3, piece, dims, preferred_element_type=F32)
            acc = part if acc is None else acc + part
        pacc_ref[...] += acc

    wait_zy(0)
    make_g(0, g0_ref)

    def pair(i, carry):
        for k, (now, later) in enumerate(((g0_ref, g1_ref), (g1_ref, g0_ref))):
            c = 2 * i + k

            @pl.when(c + AHEAD < N_CHUNK)
            def _():
                start(c + AHEAD)

            wait_zy(c + 1)
            wait_e(c)
            make_g(c + 1, later)
            use_g(c, now)
        return carry

    lax.fori_loop(0, N_CHUNK // 2, pair, 0)
    wait_e(N_CHUNK - 1)
    use_g(N_CHUNK - 1, g0_ref)

    pacc = pacc_ref[...]
    p_all[me] = pacc[0:8] + pacc[8:16] + pacc[16:24]
    pl.semaphore_wait(barrier, GROUP - 1)

    def p_copy(d):
        return pltpu.make_async_remote_copy(
            src_ref=p_all.at[me], dst_ref=p_all.at[me], send_sem=sem_ps.at[d], recv_sem=sem_pr.at[d],
            device_id=(lax.rem(me + d, GROUP),), device_id_type=MESH)

    for d in range(1, GROUP):
        p_copy(d).start()
    for d in range(1, GROUP):
        p_copy(d).wait()
    p_sum = p_all[0]
    for d in range(1, GROUP):
        p_sum = p_sum + p_all[d]
    p_t = orthonormal_rows(p_sum)
    pt_ref[...] = p_t
    p3 = stack3(p_t)

    def q_block(half, off, width):
        cols = pl.ds(pl.multiple_of(half * HALF + off, 128), width)
        acc = None
        for piece in split3(m_ref[:, cols]):
            part = jnp.dot(p3, piece, preferred_element_type=F32)
            acc = part if acc is None else acc + part
        return acc[0:8] + acc[8:16] + acc[16:24]

    for off, width in PIECES:
        q_part[:, off:off + width] = q_block(1 - core, off, width)
    to_mate = pltpu.make_async_remote_copy(
        src_ref=q_part, dst_ref=q_pair, send_sem=sem_q1.at[0], recv_sem=sem_q1.at[1],
        device_id=(mate,), device_id_type=MESH)
    to_mate.start()
    own = [q_block(core, off, width) for off, width in PIECES]
    to_mate.wait()
    for (off, width), val in zip(PIECES, own):
        q_all[chip, :, off:off + width] = val + q_pair[:, off:off + width]

    def q_copy(d):
        return pltpu.make_async_remote_copy(
            src_ref=q_all.at[chip], dst_ref=q_all.at[chip], send_sem=sem_q2s.at[d], recv_sem=sem_q2r.at[d],
            device_id=(lax.rem(me + 2 * d, GROUP),), device_id_type=MESH)

    for d in range(1, 4):
        q_copy(d).start()
    for d in range(1, 4):
        q_copy(d).wait()
    my_half = pl.ds(pl.multiple_of(core * HALF, 128), HALF)
    qn_ref[:, my_half] = (q_all[0] + q_all[1] + q_all[2] + q_all[3]) * (1.0 / GROUP)
    done = pltpu.make_async_remote_copy(
        src_ref=qn_ref.at[:, my_half], dst_ref=qn_ref.at[:, my_half], send_sem=sem_q3.at[0],
        recv_sem=sem_q3.at[1], device_id=(mate,), device_id_type=MESH)
    done.start()
    done.wait()


def error_kernel(pt_ref, qn_ref, m_ref, e_ref, po_ref, qo_ref):
    @pl.when(pl.program_id(0) == 0)
    def _():
        po_ref[...] = pt_ref[...]

    qo_ref[...] = qn_ref[...]

    def order(parts):
        return jnp.concatenate([p.astype(F32) for p in parts], axis=0).astype(BF16)

    ph, pm, pl_ = split3(pt_ref[...])
    qh, qm, ql = split3(qn_ref[...])
    left = order((ph, ph, ph, pm, pm, pl_))
    right = order((qh, qm, ql, qh, qm, qh))
    est = lax.dot_general(left, right, (((0,), (0,)), ((), ())), preferred_element_type=F32)
    cols = pl.ds(pl.multiple_of(pl.program_id(0) * e_ref.shape[1], 128), e_ref.shape[1])
    e_ref[...] = m_ref[:, cols] - est


def per_device(act_in, pre_act, grad_out, q_init, err_mem):
    vm = pl.BlockSpec(memory_space=pltpu.VMEM)
    anyspec = pl.BlockSpec(memory_space=pl.ANY)
    merged, p_t, qn_t = pl.pallas_call(
        main_kernel,
        out_shape=(pltpu.VMEM((D_IN, D_OUT), F32), pltpu.VMEM((RANK, D_IN), F32), pltpu.VMEM((RANK, D_OUT), F32)),
        in_specs=[vm, anyspec, anyspec, vm, anyspec],
        out_specs=(vm, vm, vm),
        scratch_shapes=[
            pltpu.VMEM((ROWS, D_OUT), BF16),
            pltpu.VMEM((ROWS, D_OUT), BF16),
            pltpu.VMEM((D_IN, ROWS), BF16),
            pltpu.VMEM((ROWS, CHUNK), BF16),
            pltpu.VMEM((ROWS, CHUNK), BF16),
            pltpu.VMEM((3 * RANK, D_IN), F32),
            pltpu.VMEM((GROUP, RANK, D_IN), F32),
            pltpu.VMEM((RANK, HALF), F32),
            pltpu.VMEM((RANK, HALF), F32),
            pltpu.VMEM((4, RANK, HALF), F32),
            pltpu.SemaphoreType.DMA((3, N_CHUNK)),
            pltpu.SemaphoreType.DMA((GROUP,)),
            pltpu.SemaphoreType.DMA((GROUP,)),
            pltpu.SemaphoreType.DMA((2,)),
            pltpu.SemaphoreType.DMA((4,)),
            pltpu.SemaphoreType.DMA((4,)),
            pltpu.SemaphoreType.DMA((2,)),
        ],
        compiler_params=pltpu.CompilerParams(
            collective_id=0, has_side_effects=True, vmem_limit_bytes=VMEM1),
        name='merge_and_factor',
    )(act_in, pre_act, grad_out, q_init.T, err_mem.reshape(D_IN, D_OUT))
    bw = 256
    err_new, p_o, qn_o = pl.pallas_call(
        error_kernel,
        grid=(D_OUT // bw,),
        out_shape=(jax.ShapeDtypeStruct((D_IN, D_OUT), F32), jax.ShapeDtypeStruct((RANK, D_IN), F32),
                   jax.ShapeDtypeStruct((RANK, D_OUT), F32)),
        in_specs=[pl.BlockSpec((RANK, D_IN), lambda i: (0, 0)), pl.BlockSpec((RANK, bw), lambda i: (0, i)),
                  vm],
        out_specs=(pl.BlockSpec((D_IN, bw), lambda i: (0, i)), pl.BlockSpec((RANK, D_IN), lambda i: (0, 0)),
                   pl.BlockSpec((RANK, bw), lambda i: (0, i))),
        compiler_params=pltpu.CompilerParams(vmem_limit_bytes=VMEM2),
        name='new_error',
    )(p_t, qn_t, merged)
    return p_o.T, qn_o.T, err_new[None]


VMEM1 = 44 * 1024 * 1024
VMEM2 = 24 * 1024 * 1024


def solution(mesh):
    return jax.shard_map(
        per_device, mesh=mesh,
        in_specs=(P('data', None), P('data', None), P('data', None), P(None, None), P('data', None, None)),
        out_specs=(P(None, None), P(None, None), P('data', None, None)), check_vma=False)
```

```python
import jax
import jax.numpy as jnp
from jax import lax
from jax.experimental import pallas as pl
from jax.experimental.pallas import tpu as pltpu
from jax.sharding import PartitionSpec as P

F32 = jnp.float32
BF16 = jnp.bfloat16
GROUP = 8
ROWS = 1024
D_IN = 896
D_OUT = 4864
RANK = 8
LANES = 128
CHUNK = 256
N_CHUNK = D_OUT // CHUNK
HALF = D_OUT // 2
SIDE = D_IN // 2
SLAB = 64
SLABS = SIDE // SLAB
PADDED = 4 * RANK
AHEAD = 6
MESH = pl.DeviceIdType.MESH
C0 = 0.7978845608028654
C1 = 0.044715
VMEM_MERGE = 44 * 1024 * 1024
VMEM_FACTOR = 20 * 1024 * 1024
VMEM_ERROR = 20 * 1024 * 1024


def split3(x):
    hi = x.astype(BF16)
    rest = x - hi.astype(F32)
    mid = rest.astype(BF16)
    low = (rest - mid.astype(F32)).astype(BF16)
    return hi, mid, low


def stacked(parts):
    return jnp.concatenate([p.astype(F32) for p in parts], axis=0).astype(BF16)


def gelu_grad_times(z, dy):
    x = z.astype(F32)
    sq = x * x
    s = lax.logistic(x * (2.0 * C0 + (2.0 * C0 * C1) * sq))
    r = 2.0 * C0 + (6.0 * C0 * C1) * sq
    return (s * (1.0 + ((1.0 - s) * x) * r) * dy.astype(F32)).astype(BF16)


def orthonormal_rows(p0):
    p0 = p0 / jnp.max(jnp.abs(p0), axis=1, keepdims=True)
    row = lax.broadcasted_iota(jnp.int32, (RANK, 1), 0)
    cur = p0
    for k in range(RANK):
        v = jnp.broadcast_to(cur[k:k + 1, :], cur.shape)
        inv = lax.rsqrt(jnp.sum(v * v, axis=1, keepdims=True))
        coef = jnp.sum(v * p0, axis=1, keepdims=True) * inv
        q = v * inv
        cur = jnp.where(row == k, q, cur - jnp.where(row > k, coef, 0.0) * q)
    return cur


def wide(ref, first, rows):
    return jnp.concatenate([ref[first, rows, :], ref[first + 1, rows, :]], axis=1)


def merge_kernel(a_hbm, z_hbm, dy_hbm, qt_ref, e_hbm, m_ref, p_ref,
                 a_v, z_v, dy_v, at_ref, g0, g1, pc0, pc1, sem_in, sem_a):
    gs = (g0, g1)
    pieces = (pc0, pc1)

    def cols_of(c):
        return pl.ds(c * CHUNK if isinstance(c, int) else pl.multiple_of(c * CHUNK, CHUNK), CHUNK)

    def copy(k, c):
        src, dst = ((z_hbm, z_v), (dy_hbm, dy_v), (e_hbm, m_ref))[k]
        return pltpu.make_async_copy(src.at[:, cols_of(c)], dst.at[:, cols_of(c)], sem_in.at[k, c])

    def start(c):
        for k in range(3):
            copy(k, c).start()

    def gelu_slab(c, j):
        rows = pl.ds(j * SLAB, SLAB)
        g = gelu_grad_times(z_v[rows, cols_of(c)], dy_v[rows, cols_of(c)])
        for b in range(2):
            gs[c_par(c)][b, rows, :] = g[:, b * LANES:(b + 1) * LANES]

    par_box = [0]

    def c_par(c):
        return par_box[0] ^ 1

    def body_of(accs, p_acc):
        def merge_slab(c, par, q, i):
            rows = pl.ds(q * SIDE + i * SLAB, SLAB)
            m = pltpu.matmul_pop(accs[par][q][i]) * (1.0 / ROWS) + m_ref[rows, cols_of(c)]
            m_ref[rows, cols_of(c)] = m
            for t, piece in enumerate(split3(m)):
                for b in range(2):
                    pieces[par][t, b, rows, :] = piece[:, b * LANES:(b + 1) * LANES]

        def grad_step(par, q, k):
            pltpu.matmul_push_rhs(wide(gs[par], 0, pl.ds(k * CHUNK, CHUNK)), staging_register=0, mxu_index=q)
            for i in range(SLABS):
                lhs = wide(at_ref, 2 * k, pl.ds(q * SIDE + i * SLAB, SLAB))
                pltpu.matmul_acc_lhs(accs[par][q][i], lhs, load_staged_rhs=0 if i == 0 else None)

        def rank_step(q3, par, q, blk, t):
            rows = pl.ds(q * SIDE + blk * (SIDE - CHUNK), CHUNK)
            tile = jnp.concatenate([pieces[par][t, 0, rows, :], pieces[par][t, 1, rows, :]], axis=1)
            pltpu.matmul_push_rhs(tile, staging_register=1, mxu_index=q, transpose=True)
            pltpu.matmul_acc_lhs(p_acc[q][blk], q3, load_staged_rhs=1)

        def step(c, par, gelu, grad, merge, rank):
            par_box[0] = par
            if gelu:
                copy(0, c + 1).wait()
                copy(1, c + 1).wait()
            if merge:
                copy(2, c - 1).wait()
            if rank:
                qt = qt_ref[:, cols_of(c - 2)]
                q3 = stacked(split3(qt) + (jnp.zeros_like(qt),))
            tiles = [(blk, t) for blk in range(2) for t in range(3)]
            mxu = []
            for k in range(4):
                if grad:
                    mxu.append(lambda q, k=k: grad_step(par, q, k))
                for n, (blk, t) in enumerate(tiles):
                    if rank and n * 4 // len(tiles) == k:
                        mxu.append(lambda q, blk=blk, t=t: rank_step(q3, par, q, blk, t))
            n_gelu = ROWS // SLAB
            for s in range(SLABS):
                for n, op in enumerate(mxu):
                    if n * SLABS // len(mxu) == s:
                        op(0)
                        op(1)
                if merge:
                    merge_slab(c - 1, par ^ 1, 0, s)
                    merge_slab(c - 1, par ^ 1, 1, s)
                if gelu:
                    for j in range(n_gelu):
                        if j * SLABS // n_gelu == s:
                            gelu_slab(c + 1, j)

        load_a = pltpu.make_async_copy(a_hbm, a_v, sem_a)
        load_a.start()
        for c in range(AHEAD):
            start(c)
        load_a.wait()
        for b in range(ROWS // LANES):
            at_ref[b] = a_v[b * LANES:(b + 1) * LANES, :].T
        step(-1, 1, True, False, False, False)
        start(AHEAD)
        step(0, 0, True, True, False, False)
        start(AHEAD + 1)
        step(1, 1, True, True, True, False)

        def pair(i, carry):
            for par in range(2):
                c = 2 * i + par

                @pl.when(c + AHEAD < N_CHUNK)
                def _():
                    start(c + AHEAD)

                step(c, par, True, True, True, True)
            return carry

        lax.fori_loop(1, N_CHUNK // 2, pair, 0)
        step(N_CHUNK - 1, 0, False, True, True, True)
        step(N_CHUNK, 1, False, False, True, True)
        step(N_CHUNK + 1, 0, False, False, False, True)
        skip = 2 * CHUNK - SIDE
        out = []
        for q in range(2):
            for blk in range(2):
                p3 = pltpu.matmul_pop(p_acc[q][blk])
                part = p3[0:8] + p3[8:16] + p3[16:24]
                out.append(part[:, skip:] if blk else part)
        p_ref[...] = jnp.concatenate(out, axis=1)

    def acc(q, rows):
        return pltpu.ACC(q)((rows, CHUNK), F32)

    pl.run_scoped(
        body_of,
        tuple(tuple(tuple(acc(q, SLAB) for _ in range(SLABS)) for q in range(2)) for _ in range(2)),
        tuple(tuple(acc(q, PADDED) for _ in range(2)) for q in range(2)))


def factor_kernel(p_ref, m_ref, pt_ref, qn_ref, p_all, pc0, pc1, q_part, q_pair, q_all,
                  sem_ps, sem_pr, sem_q1, sem_q2s, sem_q2r, sem_q3):
    me = lax.axis_index('data')
    core = lax.rem(me, 2)
    chip = me // 2
    mate = me + 1 - 2 * core
    pieces = (pc0, pc1)

    barrier = pltpu.get_barrier_semaphore()
    for d in range(1, GROUP):
        pl.semaphore_signal(barrier, inc=1, device_id=(lax.rem(me + d, GROUP),), device_id_type=MESH)
    p_all[me] = p_ref[...]
    pl.semaphore_wait(barrier, GROUP - 1)

    def p_copy(d):
        return pltpu.make_async_remote_copy(
            src_ref=p_ref, dst_ref=p_all.at[me], send_sem=sem_ps.at[d], recv_sem=sem_pr.at[d],
            device_id=(lax.rem(me + d, GROUP),), device_id_type=MESH)

    for d in range(1, GROUP):
        p_copy(d).start()
    for d in range(1, GROUP):
        p_copy(d).wait()
    p_sum = p_all[0]
    for d in range(1, GROUP):
        p_sum = p_sum + p_all[d]
    p_t = orthonormal_rows(p_sum)
    pt_ref[...] = p_t
    p3 = stacked(split3(p_t))

    def split_block(half, off, width, par):
        cols = pl.ds(pl.multiple_of(half * HALF + off, LANES), width)
        for r in range(0, D_IN, SLAB):
            rows = pl.ds(r, SLAB)
            for t, piece in enumerate(split3(m_ref[rows, cols])):
                for b in range(width // LANES):
                    pieces[par][t, b, rows, :] = piece[:, b * LANES:(b + 1) * LANES]

    def q_block(width, par):
        acc = None
        for t in range(3):
            tile = jnp.concatenate([pieces[par][t, b] for b in range(width // LANES)], axis=1)
            part = jnp.dot(p3, tile, preferred_element_type=F32)
            acc = part if acc is None else acc + part
        return acc[0:8] + acc[8:16] + acc[16:24]

    blocks = [(off, min(CHUNK, HALF - off)) for off in range(0, HALF, CHUNK)]
    work = [(1 - core, off, width) for off, width in blocks] + [(core, off, width) for off, width in blocks]
    to_mate = pltpu.make_async_remote_copy(
        src_ref=q_part, dst_ref=q_pair, send_sem=sem_q1.at[0], recv_sem=sem_q1.at[1],
        device_id=(mate,), device_id_type=MESH)
    own = []
    split_block(*work[0], 0)
    for n, (half, off, width) in enumerate(work):
        if n + 1 < len(work):
            split_block(*work[n + 1], (n + 1) % 2)
        val = q_block(width, n % 2)
        if n < len(blocks):
            q_part[:, off:off + width] = val
            if n == len(blocks) - 1:
                to_mate.start()
        else:
            own.append(val)
    to_mate.wait()
    for (off, width), val in zip(blocks, own):
        q_all[chip, :, off:off + width] = val + q_pair[:, off:off + width]

    def q_copy(d):
        return pltpu.make_async_remote_copy(
            src_ref=q_all.at[chip], dst_ref=q_all.at[chip], send_sem=sem_q2s.at[d], recv_sem=sem_q2r.at[d],
            device_id=(lax.rem(me + 2 * d, GROUP),), device_id_type=MESH)

    for d in range(1, 4):
        q_copy(d).start()
    for d in range(1, 4):
        q_copy(d).wait()
    my_half = pl.ds(pl.multiple_of(core * HALF, LANES), HALF)
    qn_ref[:, my_half] = (q_all[0] + q_all[1] + q_all[2] + q_all[3]) * (1.0 / GROUP)
    done = pltpu.make_async_remote_copy(
        src_ref=qn_ref.at[:, my_half], dst_ref=qn_ref.at[:, my_half], send_sem=sem_q3.at[0],
        recv_sem=sem_q3.at[1], device_id=(mate,), device_id_type=MESH)
    done.start()
    done.wait()


def error_kernel(pt_ref, qn_ref, m_ref, e_ref, po_ref, qo_ref, left_ref, right_ref):
    @pl.when(pl.program_id(0) == 0)
    def _():
        po_ref[...] = pt_ref[...]
        qo_ref[...] = qn_ref[...]
        ph, pm, pl_ = split3(pt_ref[...])
        qh, qm, ql = split3(qn_ref[...])
        left_ref[...] = stacked((ph, ph, ph, pm, pm, pl_)).T
        right_ref[...] = stacked((qh, qm, ql, qh, qm, qh))

    n = e_ref.shape[0]
    rows = pl.ds(pl.multiple_of(pl.program_id(0) * n, 16), n)
    est = jnp.dot(left_ref[rows, :], right_ref[...], preferred_element_type=F32)
    e_ref[...] = m_ref[rows, :] - est


def per_device(act_in, pre_act, grad_out, q_init, err_mem):
    vm = pl.BlockSpec(memory_space=pltpu.VMEM)
    anyspec = pl.BlockSpec(memory_space=pl.ANY)
    merged, p_part = pl.pallas_call(
        merge_kernel,
        out_shape=(pltpu.VMEM((D_IN, D_OUT), F32), pltpu.VMEM((RANK, D_IN), F32)),
        in_specs=[anyspec, anyspec, anyspec, vm, anyspec],
        out_specs=(vm, vm),
        scratch_shapes=[
            pltpu.VMEM((ROWS, D_IN), BF16),
            pltpu.VMEM((ROWS, D_OUT), BF16),
            pltpu.VMEM((ROWS, D_OUT), BF16),
            pltpu.VMEM((ROWS // LANES, D_IN, LANES), BF16),
            pltpu.VMEM((2, ROWS, LANES), BF16),
            pltpu.VMEM((2, ROWS, LANES), BF16),
            pltpu.VMEM((3, 2, D_IN, LANES), BF16),
            pltpu.VMEM((3, 2, D_IN, LANES), BF16),
            pltpu.SemaphoreType.DMA((3, N_CHUNK)),
            pltpu.SemaphoreType.DMA,
        ],
        compiler_params=pltpu.CompilerParams(vmem_limit_bytes=VMEM_MERGE),
        name='merge',
    )(act_in, pre_act, grad_out, q_init.T, err_mem.reshape(D_IN, D_OUT))
    p_t, qn_t = pl.pallas_call(
        factor_kernel,
        out_shape=(pltpu.VMEM((RANK, D_IN), F32), pltpu.VMEM((RANK, D_OUT), F32)),
        in_specs=[vm, vm],
        out_specs=(vm, vm),
        scratch_shapes=[
            pltpu.VMEM((GROUP, RANK, D_IN), F32),
            pltpu.VMEM((3, 2, D_IN, LANES), BF16),
            pltpu.VMEM((3, 2, D_IN, LANES), BF16),
            pltpu.VMEM((RANK, HALF), F32),
            pltpu.VMEM((RANK, HALF), F32),
            pltpu.VMEM((4, RANK, HALF), F32),
            pltpu.SemaphoreType.DMA((GROUP,)),
            pltpu.SemaphoreType.DMA((GROUP,)),
            pltpu.SemaphoreType.DMA((2,)),
            pltpu.SemaphoreType.DMA((4,)),
            pltpu.SemaphoreType.DMA((4,)),
            pltpu.SemaphoreType.DMA((2,)),
        ],
        compiler_params=pltpu.CompilerParams(
            collective_id=0, has_side_effects=True, vmem_limit_bytes=VMEM_FACTOR),
        name='factor',
    )(p_part, merged)
    bh = 112
    err_new, p_o, qn_o = pl.pallas_call(
        error_kernel,
        grid=(D_IN // bh,),
        out_shape=(jax.ShapeDtypeStruct((D_IN, D_OUT), F32), jax.ShapeDtypeStruct((RANK, D_IN), F32),
                   jax.ShapeDtypeStruct((RANK, D_OUT), F32)),
        in_specs=[vm, vm, vm],
        out_specs=(pl.BlockSpec((bh, D_OUT), lambda i: (i, 0)), pl.BlockSpec((RANK, D_IN), lambda i: (0, 0)),
                   pl.BlockSpec((RANK, D_OUT), lambda i: (0, 0))),
        scratch_shapes=[pltpu.VMEM((D_IN, 6 * RANK), BF16), pltpu.VMEM((6 * RANK, D_OUT), BF16)],
        compiler_params=pltpu.CompilerParams(vmem_limit_bytes=VMEM_ERROR),
        name='new_error',
    )(p_t, qn_t, merged)
    return p_o.T, qn_o.T, err_new[None]


def solution(mesh):
    return jax.shard_map(
        per_device, mesh=mesh,
        in_specs=(P('data', None), P('data', None), P('data', None), P(None, None), P('data', None, None)),
        out_specs=(P(None, None), P(None, None), P('data', None, None)), check_vma=False)
```

```python
import jax
import jax.numpy as jnp
from jax import lax
from jax.experimental import pallas as pl
from jax.experimental.pallas import tpu as pltpu
from jax.sharding import PartitionSpec as P

F32 = jnp.float32
BF16 = jnp.bfloat16
GROUP = 8
ROWS = 1024
D_IN = 896
D_OUT = 4864
RANK = 8
LANES = 128
CHUNK = 256
N_CHUNK = D_OUT // CHUNK
HALF = D_OUT // 2
SIDE = D_IN // 2
SLAB = 64
SLABS = SIDE // SLAB
PADDED = 4 * RANK
AHEAD = 6
MESH = pl.DeviceIdType.MESH
C0 = 0.7978845608028654
C1 = 0.044715
VMEM_MERGE = 44 * 1024 * 1024
VMEM_FACTOR = 20 * 1024 * 1024
VMEM_ERROR = 20 * 1024 * 1024


def split3(x):
    hi = x.astype(BF16)
    rest = x - hi.astype(F32)
    mid = rest.astype(BF16)
    low = (rest - mid.astype(F32)).astype(BF16)
    return hi, mid, low


def stacked(parts):
    return jnp.concatenate([p.astype(F32) for p in parts], axis=0).astype(BF16)


def gelu_grad_times(z, dy):
    x = z.astype(F32)
    sq = x * x
    s = lax.logistic(x * (2.0 * C0 + (2.0 * C0 * C1) * sq))
    r = 2.0 * C0 + (6.0 * C0 * C1) * sq
    return (s * (1.0 + ((1.0 - s) * x) * r) * dy.astype(F32)).astype(BF16)


def orthonormal_rows(p0):
    p0 = p0 / jnp.max(jnp.abs(p0), axis=1, keepdims=True)
    row = lax.broadcasted_iota(jnp.int32, (RANK, 1), 0)
    cur = p0
    for k in range(RANK):
        v = jnp.broadcast_to(cur[k:k + 1, :], cur.shape)
        inv = lax.rsqrt(jnp.sum(v * v, axis=1, keepdims=True))
        coef = jnp.sum(v * p0, axis=1, keepdims=True) * inv
        q = v * inv
        cur = jnp.where(row == k, q, cur - jnp.where(row > k, coef, 0.0) * q)
    return cur


def wide(ref, first, rows):
    return jnp.concatenate([ref[first, rows, :], ref[first + 1, rows, :]], axis=1)


def merge_kernel(a_hbm, z_hbm, dy_hbm, qt_ref, e_hbm, m_ref, p_ref,
                 a_v, z_v, dy_v, at_ref, q3_v, g0, g1, pc0, pc1, sem_in, sem_a):
    gs = (g0, g1)
    pieces = (pc0, pc1)

    def cols_of(c):
        return pl.ds(c * CHUNK if isinstance(c, int) else pl.multiple_of(c * CHUNK, CHUNK), CHUNK)

    def copy(k, c):
        src, dst = ((z_hbm, z_v), (dy_hbm, dy_v), (e_hbm, m_ref))[k]
        return pltpu.make_async_copy(src.at[:, cols_of(c)], dst.at[:, cols_of(c)], sem_in.at[k, c])

    def start(c):
        for k in range(3):
            copy(k, c).start()

    def gelu_slab(c, j):
        rows = pl.ds(j * SLAB, SLAB)
        g = gelu_grad_times(z_v[rows, cols_of(c)], dy_v[rows, cols_of(c)])
        for b in range(2):
            gs[c_par(c)][b, rows, :] = g[:, b * LANES:(b + 1) * LANES]

    par_box = [0]

    def c_par(c):
        return par_box[0] ^ 1

    def body_of(accs, p_acc):
        def merge_slab(c, par, q, i):
            rows = pl.ds(q * SIDE + i * SLAB, SLAB)
            m = pltpu.matmul_pop(accs[par][q][i]) * (1.0 / ROWS) + m_ref[rows, cols_of(c)]
            m_ref[rows, cols_of(c)] = m
            for t, piece in enumerate(split3(m)):
                for b in range(2):
                    pieces[par][t, b, rows, :] = piece[:, b * LANES:(b + 1) * LANES]

        def grad_step(par, q, k):
            pltpu.matmul_push_rhs(wide(gs[par], 0, pl.ds(k * CHUNK, CHUNK)), staging_register=0, mxu_index=q)
            for i in range(SLABS):
                lhs = wide(at_ref, 2 * k, pl.ds(q * SIDE + i * SLAB, SLAB))
                pltpu.matmul_acc_lhs(accs[par][q][i], lhs, load_staged_rhs=0 if i == 0 else None)

        def rank_step(q3, par, q, blk, t):
            rows = pl.ds(q * SIDE + blk * (SIDE - CHUNK), CHUNK)
            tile = jnp.concatenate([pieces[par][t, 0, rows, :], pieces[par][t, 1, rows, :]], axis=1)
            pltpu.matmul_push_rhs(tile, staging_register=1, mxu_index=q, transpose=True)
            pltpu.matmul_acc_lhs(p_acc[q][blk], q3, load_staged_rhs=1)

        def step(c, par, gelu, grad, merge, rank):
            par_box[0] = par
            if gelu:
                copy(0, c + 1).wait()
                copy(1, c + 1).wait()
            if merge:
                copy(2, c - 1).wait()
            if rank:
                q3 = jnp.concatenate([q3_v[2 * (c - 2)], q3_v[2 * (c - 2) + 1]], axis=1)
            tiles = [(blk, t) for blk in range(2) for t in range(3)]
            mxu = []
            for k in range(4):
                if grad:
                    mxu.append(lambda q, k=k: grad_step(par, q, k))
                for n, (blk, t) in enumerate(tiles):
                    if rank and n * 4 // len(tiles) == k:
                        mxu.append(lambda q, blk=blk, t=t: rank_step(q3, par, q, blk, t))
            n_gelu = ROWS // SLAB
            if merge:
                for s in range(SLABS):
                    merge_slab(c - 1, par ^ 1, 0, s)
                    merge_slab(c - 1, par ^ 1, 1, s)
            for s in range(SLABS):
                for n, op in enumerate(mxu):
                    if n * SLABS // len(mxu) == s:
                        op(0)
                        op(1)
                if gelu:
                    for j in range(n_gelu):
                        if j * SLABS // n_gelu == s:
                            gelu_slab(c + 1, j)

        load_a = pltpu.make_async_copy(a_hbm, a_v, sem_a)
        load_a.start()
        for c in range(AHEAD):
            start(c)
        qt = qt_ref[...]
        q_all = stacked(split3(qt) + (jnp.zeros_like(qt),))
        for b in range(2 * N_CHUNK):
            q3_v[b] = q_all[:, b * LANES:(b + 1) * LANES]
        load_a.wait()
        copy(0, 0).wait()
        copy(1, 0).wait()
        par_box[0] = 1
        for b in range(ROWS // LANES):
            at_ref[b] = a_v[b * LANES:(b + 1) * LANES, :].T
            gelu_slab(0, 2 * b)
            gelu_slab(0, 2 * b + 1)
        start(AHEAD)
        step(0, 0, True, True, False, False)
        start(AHEAD + 1)
        step(1, 1, True, True, True, False)

        def pair(i, carry):
            for par in range(2):
                c = 2 * i + par

                @pl.when(c + AHEAD < N_CHUNK)
                def _():
                    start(c + AHEAD)

                @pl.when(c + 1 < N_CHUNK)
                def _():
                    step(c, par, True, True, True, True)
            return carry

        lax.fori_loop(1, N_CHUNK // 2, pair, 0)
        step(N_CHUNK - 1, 0, False, True, True, True)
        step(N_CHUNK, 1, False, False, True, True)
        step(N_CHUNK + 1, 0, False, False, False, True)
        skip = 2 * CHUNK - SIDE
        out = []
        for q in range(2):
            for blk in range(2):
                p3 = pltpu.matmul_pop(p_acc[q][blk])
                part = p3[0:8] + p3[8:16] + p3[16:24]
                out.append(part[:, skip:] if blk else part)
        p_ref[...] = jnp.concatenate(out, axis=1)

    def acc(q, rows):
        return pltpu.ACC(q)((rows, CHUNK), F32)

    pl.run_scoped(
        body_of,
        tuple(tuple(tuple(acc(q, SLAB) for _ in range(SLABS)) for q in range(2)) for _ in range(2)),
        tuple(tuple(acc(q, PADDED) for _ in range(2)) for q in range(2)))


def factor_kernel(p_ref, m_ref, pt_ref, qn_ref, p_all, pc0, pc1, q_part, q_pair, q_all,
                  sem_ps, sem_pr, sem_q1, sem_q2s, sem_q2r, sem_q3):
    me = lax.axis_index('data')
    core = lax.rem(me, 2)
    chip = me // 2
    mate = me + 1 - 2 * core
    pieces = (pc0, pc1)

    barrier = pltpu.get_barrier_semaphore()
    for d in range(1, GROUP):
        pl.semaphore_signal(barrier, inc=1, device_id=(lax.rem(me + d, GROUP),), device_id_type=MESH)
    p_all[me] = p_ref[...]
    pl.semaphore_wait(barrier, GROUP - 1)

    def p_copy(d):
        return pltpu.make_async_remote_copy(
            src_ref=p_ref, dst_ref=p_all.at[me], send_sem=sem_ps.at[d], recv_sem=sem_pr.at[d],
            device_id=(lax.rem(me + d, GROUP),), device_id_type=MESH)

    for d in range(1, GROUP):
        p_copy(d).start()
    for d in range(1, GROUP):
        p_copy(d).wait()
    p_sum = p_all[0]
    for d in range(1, GROUP):
        p_sum = p_sum + p_all[d]
    p_t = orthonormal_rows(p_sum)
    pt_ref[...] = p_t
    p3 = stacked(split3(p_t))

    def split_block(half, off, width, par):
        cols = pl.ds(pl.multiple_of(half * HALF + off, LANES), width)
        for r in range(0, D_IN, SLAB):
            rows = pl.ds(r, SLAB)
            for t, piece in enumerate(split3(m_ref[rows, cols])):
                for b in range(width // LANES):
                    pieces[par][t, b, rows, :] = piece[:, b * LANES:(b + 1) * LANES]

    def q_block(width, par):
        acc = None
        for t in range(3):
            tile = jnp.concatenate([pieces[par][t, b] for b in range(width // LANES)], axis=1)
            part = jnp.dot(p3, tile, preferred_element_type=F32)
            acc = part if acc is None else acc + part
        return acc[0:8] + acc[8:16] + acc[16:24]

    blocks = [(off, min(CHUNK, HALF - off)) for off in range(0, HALF, CHUNK)]
    work = [(1 - core, off, width) for off, width in blocks] + [(core, off, width) for off, width in blocks]
    to_mate = pltpu.make_async_remote_copy(
        src_ref=q_part, dst_ref=q_pair, send_sem=sem_q1.at[0], recv_sem=sem_q1.at[1],
        device_id=(mate,), device_id_type=MESH)
    own = []
    split_block(*work[0], 0)
    for n, (half, off, width) in enumerate(work):
        if n + 1 < len(work):
            split_block(*work[n + 1], (n + 1) % 2)
        val = q_block(width, n % 2)
        if n < len(blocks):
            q_part[:, off:off + width] = val
            if n == len(blocks) - 1:
                to_mate.start()
        else:
            own.append(val)
    to_mate.wait()
    for (off, width), val in zip(blocks, own):
        q_all[chip, :, off:off + width] = val + q_pair[:, off:off + width]

    def q_copy(d):
        return pltpu.make_async_remote_copy(
            src_ref=q_all.at[chip], dst_ref=q_all.at[chip], send_sem=sem_q2s.at[d], recv_sem=sem_q2r.at[d],
            device_id=(lax.rem(me + 2 * d, GROUP),), device_id_type=MESH)

    for d in range(1, 4):
        q_copy(d).start()
    for d in range(1, 4):
        q_copy(d).wait()
    my_half = pl.ds(pl.multiple_of(core * HALF, LANES), HALF)
    qn_ref[:, my_half] = (q_all[0] + q_all[1] + q_all[2] + q_all[3]) * (1.0 / GROUP)
    done = pltpu.make_async_remote_copy(
        src_ref=qn_ref.at[:, my_half], dst_ref=qn_ref.at[:, my_half], send_sem=sem_q3.at[0],
        recv_sem=sem_q3.at[1], device_id=(mate,), device_id_type=MESH)
    done.start()
    done.wait()


def error_kernel(pt_ref, qn_ref, m_ref, e_ref, po_ref, qo_ref, left_ref, right_ref):
    @pl.when(pl.program_id(0) == 0)
    def _():
        po_ref[...] = pt_ref[...]
        qo_ref[...] = qn_ref[...]
        ph, pm, pl_ = split3(pt_ref[...])
        qh, qm, ql = split3(qn_ref[...])
        left_ref[...] = stacked((ph, ph, ph, pm, pm, pl_)).T
        right_ref[...] = stacked((qh, qm, ql, qh, qm, qh))

    n = e_ref.shape[0]
    rows = pl.ds(pl.multiple_of(pl.program_id(0) * n, 16), n)
    est = jnp.dot(left_ref[rows, :], right_ref[...], preferred_element_type=F32)
    e_ref[...] = m_ref[rows, :] - est


def per_device(act_in, pre_act, grad_out, q_init, err_mem):
    vm = pl.BlockSpec(memory_space=pltpu.VMEM)
    anyspec = pl.BlockSpec(memory_space=pl.ANY)
    merged, p_part = pl.pallas_call(
        merge_kernel,
        out_shape=(pltpu.VMEM((D_IN, D_OUT), F32), pltpu.VMEM((RANK, D_IN), F32)),
        in_specs=[anyspec, anyspec, anyspec, vm, anyspec],
        out_specs=(vm, vm),
        scratch_shapes=[
            pltpu.VMEM((ROWS, D_IN), BF16),
            pltpu.VMEM((ROWS, D_OUT), BF16),
            pltpu.VMEM((ROWS, D_OUT), BF16),
            pltpu.VMEM((ROWS // LANES, D_IN, LANES), BF16),
            pltpu.VMEM((2 * N_CHUNK, PADDED, LANES), BF16),
            pltpu.VMEM((2, ROWS, LANES), BF16),
            pltpu.VMEM((2, ROWS, LANES), BF16),
            pltpu.VMEM((3, 2, D_IN, LANES), BF16),
            pltpu.VMEM((3, 2, D_IN, LANES), BF16),
            pltpu.SemaphoreType.DMA((3, N_CHUNK)),
            pltpu.SemaphoreType.DMA,
        ],
        compiler_params=pltpu.CompilerParams(vmem_limit_bytes=VMEM_MERGE),
        name='merge',
    )(act_in, pre_act, grad_out, q_init.T, err_mem.reshape(D_IN, D_OUT))
    p_t, qn_t = pl.pallas_call(
        factor_kernel,
        out_shape=(pltpu.VMEM((RANK, D_IN), F32), pltpu.VMEM((RANK, D_OUT), F32)),
        in_specs=[vm, vm],
        out_specs=(vm, vm),
        scratch_shapes=[
            pltpu.VMEM((GROUP, RANK, D_IN), F32),
            pltpu.VMEM((3, 2, D_IN, LANES), BF16),
            pltpu.VMEM((3, 2, D_IN, LANES), BF16),
            pltpu.VMEM((RANK, HALF), F32),
            pltpu.VMEM((RANK, HALF), F32),
            pltpu.VMEM((4, RANK, HALF), F32),
            pltpu.SemaphoreType.DMA((GROUP,)),
            pltpu.SemaphoreType.DMA((GROUP,)),
            pltpu.SemaphoreType.DMA((2,)),
            pltpu.SemaphoreType.DMA((4,)),
            pltpu.SemaphoreType.DMA((4,)),
            pltpu.SemaphoreType.DMA((2,)),
        ],
        compiler_params=pltpu.CompilerParams(
            collective_id=0, has_side_effects=True, vmem_limit_bytes=VMEM_FACTOR),
        name='factor',
    )(p_part, merged)
    bh = 64
    err_new, p_o, qn_o = pl.pallas_call(
        error_kernel,
        grid=(D_IN // bh,),
        out_shape=(jax.ShapeDtypeStruct((D_IN, D_OUT), F32), jax.ShapeDtypeStruct((RANK, D_IN), F32),
                   jax.ShapeDtypeStruct((RANK, D_OUT), F32)),
        in_specs=[vm, vm, vm],
        out_specs=(pl.BlockSpec((bh, D_OUT), lambda i: (i, 0)), pl.BlockSpec((RANK, D_IN), lambda i: (0, 0)),
                   pl.BlockSpec((RANK, D_OUT), lambda i: (0, 0))),
        scratch_shapes=[pltpu.VMEM((D_IN, 6 * RANK), BF16), pltpu.VMEM((6 * RANK, D_OUT), BF16)],
        compiler_params=pltpu.CompilerParams(vmem_limit_bytes=VMEM_ERROR),
        name='new_error',
    )(p_t, qn_t, merged)
    return p_o.T, qn_o.T, err_new[None]


def solution(mesh):
    return jax.shard_map(
        per_device, mesh=mesh,
        in_specs=(P('data', None), P('data', None), P('data', None), P(None, None), P('data', None, None)),
        out_specs=(P(None, None), P(None, None), P('data', None, None)), check_vma=False)
```

```python
import jax
import jax.numpy as jnp
from jax import lax
from jax.experimental import pallas as pl
from jax.experimental.pallas import tpu as pltpu
from jax.sharding import PartitionSpec as P

F32 = jnp.float32
BF16 = jnp.bfloat16
GROUP = 8
ROWS = 1024
D_IN = 896
D_OUT = 4864
RANK = 8
LANES = 128
CHUNK = 256
N_CHUNK = D_OUT // CHUNK
HALF = D_OUT // 2
SIDE = D_IN // 2
BANDS = ((0, 32), (32, 96), (128, 128), (256, 128), (384, 128), (512, 128), (640, 128), (768, 128))
SHARES = ((0, 512), (512, 512), (1024, 512), (1536, 512), (2048, 384))
SLAB = 64
SLABS = SIDE // SLAB
PADDED = 4 * RANK
AHEAD = 18
MESH = pl.DeviceIdType.MESH
C0 = 0.7978845608028654
C1 = 0.044715
VMEM_MERGE = 44 * 1024 * 1024
VMEM_FACTOR = 20 * 1024 * 1024
VMEM_ERROR = 24 * 1024 * 1024


def split3(x):
    hi = x.astype(BF16)
    rest = x - hi.astype(F32)
    mid = rest.astype(BF16)
    low = (rest - mid.astype(F32)).astype(BF16)
    return hi, mid, low


def stacked(parts):
    return jnp.concatenate([p.astype(F32) for p in parts], axis=0).astype(BF16)


def gelu_grad_times(z, dy):
    x = z.astype(F32)
    sq = x * x
    s = lax.logistic(x * (2.0 * C0 + (2.0 * C0 * C1) * sq))
    r = 2.0 * C0 + (6.0 * C0 * C1) * sq
    return (s * (1.0 + ((1.0 - s) * x) * r) * dy.astype(F32)).astype(BF16)


def orthonormal_rows(p0):
    p0 = p0 / jnp.max(jnp.abs(p0), axis=1, keepdims=True)
    row = lax.broadcasted_iota(jnp.int32, (RANK, 1), 0)
    cur = p0
    for k in range(RANK):
        v = jnp.broadcast_to(cur[k:k + 1, :], cur.shape)
        inv = lax.rsqrt(jnp.sum(v * v, axis=1, keepdims=True))
        coef = jnp.sum(v * p0, axis=1, keepdims=True) * inv
        q = v * inv
        cur = jnp.where(row == k, q, cur - jnp.where(row > k, coef, 0.0) * q)
    return cur


def wide(ref, first, rows):
    return jnp.concatenate([ref[first, rows, :], ref[first + 1, rows, :]], axis=1)


def merge_kernel(a_hbm, z_hbm, dy_hbm, qt_ref, e_hbm, m_ref, p_ref,
                 a_v, z_v, dy_v, at_ref, q3_v, g0, g1, pc0, pc1, sem_in, sem_a):
    gs = (g0, g1)
    pieces = (pc0, pc1)

    def cols_of(c):
        return pl.ds(c * CHUNK if isinstance(c, int) else pl.multiple_of(c * CHUNK, CHUNK), CHUNK)

    def copy(k, c):
        src, dst = ((z_hbm, z_v), (dy_hbm, dy_v), (e_hbm, m_ref))[k]
        return pltpu.make_async_copy(src.at[:, cols_of(c)], dst.at[:, cols_of(c)], sem_in.at[k, c])

    def start(c):
        for k in range(3):
            copy(k, c).start()

    def gelu_slab(c, j):
        rows = pl.ds(j * SLAB, SLAB)
        g = gelu_grad_times(z_v[rows, cols_of(c)], dy_v[rows, cols_of(c)])
        for b in range(2):
            gs[c_par(c)][b, rows, :] = g[:, b * LANES:(b + 1) * LANES]

    par_box = [0]

    def c_par(c):
        return par_box[0] ^ 1

    def body_of(accs, p_acc):
        def merge_slab(c, par, q, i):
            rows = pl.ds(q * SIDE + i * SLAB, SLAB)
            m = pltpu.matmul_pop(accs[par][q][i]) * (1.0 / ROWS) + m_ref[rows, cols_of(c)]
            m_ref[rows, cols_of(c)] = m
            for t, piece in enumerate(split3(m)):
                for b in range(2):
                    pieces[par][t, b, rows, :] = piece[:, b * LANES:(b + 1) * LANES]

        def grad_step(par, q, k):
            pltpu.matmul_push_rhs(wide(gs[par], 0, pl.ds(k * CHUNK, CHUNK)), staging_register=0, mxu_index=q)
            for i in range(SLABS):
                lhs = wide(at_ref, 2 * k, pl.ds(q * SIDE + i * SLAB, SLAB))
                pltpu.matmul_acc_lhs(accs[par][q][i], lhs, load_staged_rhs=0 if i == 0 else None)

        def rank_step(q3, par, q, blk, t):
            rows = pl.ds(q * SIDE + blk * (SIDE - CHUNK), CHUNK)
            tile = jnp.concatenate([pieces[par][t, 0, rows, :], pieces[par][t, 1, rows, :]], axis=1)
            pltpu.matmul_push_rhs(tile, staging_register=1, mxu_index=q, transpose=True)
            pltpu.matmul_acc_lhs(p_acc[q][blk], q3, load_staged_rhs=1)

        def step(c, par, gelu, grad, merge, rank):
            par_box[0] = par
            if gelu:
                copy(0, c + 1).wait()
                copy(1, c + 1).wait()
            if merge:
                copy(2, c - 1).wait()
            if rank:
                q3 = jnp.concatenate([q3_v[2 * (c - 2)], q3_v[2 * (c - 2) + 1]], axis=1)
            tiles = [(blk, t) for blk in range(2) for t in range(3)]
            mxu = []
            for k in range(4):
                if grad:
                    mxu.append(lambda q, k=k: grad_step(par, q, k))
                for n, (blk, t) in enumerate(tiles):
                    if rank and n * 4 // len(tiles) == k:
                        mxu.append(lambda q, blk=blk, t=t: rank_step(q3, par, q, blk, t))
            n_gelu = ROWS // SLAB
            if merge:
                for s in range(SLABS):
                    merge_slab(c - 1, par ^ 1, 0, s)
                    merge_slab(c - 1, par ^ 1, 1, s)
            for s in range(SLABS):
                for n, op in enumerate(mxu):
                    if n * SLABS // len(mxu) == s:
                        op(0)
                        op(1)
                if gelu:
                    for j in range(n_gelu):
                        if j * SLABS // n_gelu == s:
                            gelu_slab(c + 1, j)

        load_a = pltpu.make_async_copy(a_hbm, a_v, sem_a)
        load_a.start()
        for c in range(AHEAD):
            start(c)
        qt = qt_ref[...]
        q_all = stacked(split3(qt) + (jnp.zeros_like(qt),))
        for b in range(2 * N_CHUNK):
            q3_v[b] = q_all[:, b * LANES:(b + 1) * LANES]
        load_a.wait()
        copy(0, 0).wait()
        copy(1, 0).wait()
        par_box[0] = 1
        for b in range(ROWS // LANES):
            at_ref[b] = a_v[b * LANES:(b + 1) * LANES, :].T
            gelu_slab(0, 2 * b)
            gelu_slab(0, 2 * b + 1)
        start(AHEAD)
        step(0, 0, True, True, False, False)
        step(1, 1, True, True, True, False)

        def pair(i, carry):
            for par in range(2):
                c = 2 * i + par

                @pl.when(c + 1 < N_CHUNK)
                def _():
                    step(c, par, True, True, True, True)
            return carry

        lax.fori_loop(1, N_CHUNK // 2, pair, 0)
        step(N_CHUNK - 1, 0, False, True, True, True)
        step(N_CHUNK, 1, False, False, True, True)
        step(N_CHUNK + 1, 0, False, False, False, True)
        skip = 2 * CHUNK - SIDE
        out = []
        for q in range(2):
            for blk in range(2):
                p3 = pltpu.matmul_pop(p_acc[q][blk])
                part = p3[0:8] + p3[8:16] + p3[16:24]
                out.append(part[:, skip:] if blk else part)
        p_ref[...] = jnp.concatenate(out, axis=1)

    def acc(q, rows):
        return pltpu.ACC(q)((rows, CHUNK), F32)

    pl.run_scoped(
        body_of,
        tuple(tuple(tuple(acc(q, SLAB) for _ in range(SLABS)) for q in range(2)) for _ in range(2)),
        tuple(tuple(acc(q, PADDED) for _ in range(2)) for q in range(2)))


def factor_kernel(p_ref, m_ref, pt_ref, qn_ref, p_all, p3_v, pc0, pc1, q_mine, q_part, q_pair, q_all,
                  sem_ps, sem_pr, sem_d, sem_is, sem_ir, sem_f):
    me = lax.axis_index('data')
    core = lax.rem(me, 2)
    chip = me // 2
    mate = me + 1 - 2 * core
    pieces = (pc0, pc1)

    barrier = pltpu.get_barrier_semaphore()
    for d in range(1, GROUP):
        pl.semaphore_signal(barrier, inc=1, device_id=(lax.rem(me + d, GROUP),), device_id_type=MESH)
    p_all[me] = p_ref[...]
    pl.semaphore_wait(barrier, GROUP - 1)

    def p_copy(d):
        return pltpu.make_async_remote_copy(
            src_ref=p_ref, dst_ref=p_all.at[me], send_sem=sem_ps.at[d], recv_sem=sem_pr.at[d],
            device_id=(lax.rem(me + d, GROUP),), device_id_type=MESH)

    work = []
    for g, (off, width) in enumerate(SHARES):
        for mine in range(2):
            work.append((g, mine, off, width))

    def split_block(n):
        _, mine, off, width = work[n]
        half = core if mine else 1 - core
        cols = pl.ds(pl.multiple_of(half * HALF + off, LANES), width)
        for r in range(0, D_IN, SLAB):
            rows = pl.ds(r, SLAB)
            for t, piece in enumerate(split3(m_ref[rows, cols])):
                for b in range(width // LANES):
                    pieces[n % 2][t, b, rows, :] = piece[:, b * LANES:(b + 1) * LANES]

    def rank_block(n):
        _, mine, off, width = work[n]
        p3 = jnp.concatenate([p3_v[b] for b in range(D_IN // LANES)], axis=1)
        acc = None
        for t in range(3):
            tile = jnp.concatenate([pieces[n % 2][t, b] for b in range(width // LANES)], axis=1)
            part = jnp.dot(p3, tile, preferred_element_type=F32)
            acc = part if acc is None else acc + part
        dst = q_mine if mine else q_part
        dst[:, off:off + width] = acc[0:8] + acc[8:16] + acc[16:24]

    def to_mate(g):
        cols = pl.ds(*SHARES[g])
        return pltpu.make_async_remote_copy(
            src_ref=q_part.at[:, cols], dst_ref=q_pair.at[:, cols], send_sem=sem_d.at[0, g],
            recv_sem=sem_d.at[1, g], device_id=(mate,), device_id_type=MESH)

    def to_chip(g, d):
        view = q_all.at[chip, :, pl.ds(*SHARES[g])]
        return pltpu.make_async_remote_copy(
            src_ref=view, dst_ref=view, send_sem=sem_is.at[d, g], recv_sem=sem_ir.at[d, g],
            device_id=(lax.rem(me + 2 * d, GROUP),), device_id_type=MESH)

    def my_cols(g):
        off, width = SHARES[g]
        return pl.ds(pl.multiple_of(core * HALF + off, LANES), width)

    def final(g):
        view = qn_ref.at[:, my_cols(g)]
        return pltpu.make_async_remote_copy(
            src_ref=view, dst_ref=view, send_sem=sem_f.at[0, g], recv_sem=sem_f.at[1, g],
            device_id=(mate,), device_id_type=MESH)

    def share_chip_sum(g):
        cols = pl.ds(*SHARES[g])
        to_mate(g).wait()
        q_all[chip, :, cols] = q_mine[:, cols] + q_pair[:, cols]
        for d in (2, 1, 3):
            to_chip(g, d).start()

    for d in range(1, GROUP):
        p_copy(d).start()
    split_block(0)
    for d in range(1, GROUP):
        p_copy(d).wait()
    p_sum = p_all[0]
    for d in range(1, GROUP):
        p_sum = p_sum + p_all[d]
    p_t = orthonormal_rows(p_sum)
    pt_ref[...] = p_t
    p3 = stacked(split3(p_t) + (jnp.zeros_like(p_t),))
    for b in range(D_IN // LANES):
        p3_v[b] = p3[:, b * LANES:(b + 1) * LANES]

    for n, (g, mine, off, width) in enumerate(work):
        @pl.when(me > -1 - n)
        def _(n=n):
            if n + 1 < len(work):
                split_block(n + 1)
            rank_block(n)

        last = n + 1 == len(work) or work[n + 1][:2] != (g, mine)
        if last and not mine:
            to_mate(g).start()
        if last and mine:
            if g:
                share_chip_sum(g - 1)
    share_chip_sum(len(SHARES) - 1)
    for g in range(len(SHARES)):
        cols = pl.ds(*SHARES[g])
        for d in range(1, 4):
            to_chip(g, d).wait()
        qn_ref[:, my_cols(g)] = (q_all[0, :, cols] + q_all[1, :, cols] + q_all[2, :, cols] + q_all[3, :, cols]) * (1.0 / GROUP)
        final(g).start()
    for g in range(len(SHARES)):
        final(g).wait()


def error_kernel(pt_ref, qn_ref, m_ref, e_hbm, po_ref, qo_ref, e_v, left_ref, right_ref, sem):
    po_ref[...] = pt_ref[...]
    qo_ref[...] = qn_ref[...]
    ph, pm, pl_ = split3(pt_ref[...])
    qh, qm, ql = split3(qn_ref[...])
    left_ref[...] = stacked((ph, ph, ph, pm, pm, pl_)).T
    right_ref[...] = stacked((qh, qm, ql, qh, qm, qh))

    def copy(n):
        rows = pl.ds(*BANDS[n])
        return pltpu.make_async_copy(e_v.at[rows, :], e_hbm.at[rows, :], sem.at[n])

    for n, band in enumerate(BANDS):
        rows = pl.ds(*band)
        e_v[rows, :] = m_ref[rows, :] - jnp.dot(left_ref[rows, :], right_ref[...], preferred_element_type=F32)
        copy(n).start()
    for n in range(len(BANDS)):
        copy(n).wait()


def per_device(act_in, pre_act, grad_out, q_init, err_mem):
    vm = pl.BlockSpec(memory_space=pltpu.VMEM)
    anyspec = pl.BlockSpec(memory_space=pl.ANY)
    merged, p_part = pl.pallas_call(
        merge_kernel,
        out_shape=(pltpu.VMEM((D_IN, D_OUT), F32), pltpu.VMEM((RANK, D_IN), F32)),
        in_specs=[anyspec, anyspec, anyspec, vm, anyspec],
        out_specs=(vm, vm),
        scratch_shapes=[
            pltpu.VMEM((ROWS, D_IN), BF16),
            pltpu.VMEM((ROWS, D_OUT), BF16),
            pltpu.VMEM((ROWS, D_OUT), BF16),
            pltpu.VMEM((ROWS // LANES, D_IN, LANES), BF16),
            pltpu.VMEM((2 * N_CHUNK, PADDED, LANES), BF16),
            pltpu.VMEM((2, ROWS, LANES), BF16),
            pltpu.VMEM((2, ROWS, LANES), BF16),
            pltpu.VMEM((3, 2, D_IN, LANES), BF16),
            pltpu.VMEM((3, 2, D_IN, LANES), BF16),
            pltpu.SemaphoreType.DMA((3, N_CHUNK)),
            pltpu.SemaphoreType.DMA,
        ],
        compiler_params=pltpu.CompilerParams(vmem_limit_bytes=VMEM_MERGE),
        name='merge',
    )(act_in, pre_act, grad_out, q_init.T, err_mem.reshape(D_IN, D_OUT))
    p_t, qn_t = pl.pallas_call(
        factor_kernel,
        out_shape=(pltpu.VMEM((RANK, D_IN), F32), pltpu.VMEM((RANK, D_OUT), F32)),
        in_specs=[vm, vm],
        out_specs=(vm, vm),
        scratch_shapes=[
            pltpu.VMEM((GROUP, RANK, D_IN), F32),
            pltpu.VMEM((D_IN // LANES, PADDED, LANES), BF16),
            pltpu.VMEM((3, 4, D_IN, LANES), BF16),
            pltpu.VMEM((3, 4, D_IN, LANES), BF16),
            pltpu.VMEM((RANK, HALF), F32),
            pltpu.VMEM((RANK, HALF), F32),
            pltpu.VMEM((RANK, HALF), F32),
            pltpu.VMEM((4, RANK, HALF), F32),
            pltpu.SemaphoreType.DMA((GROUP,)),
            pltpu.SemaphoreType.DMA((GROUP,)),
            pltpu.SemaphoreType.DMA((2, len(SHARES))),
            pltpu.SemaphoreType.DMA((4, len(SHARES))),
            pltpu.SemaphoreType.DMA((4, len(SHARES))),
            pltpu.SemaphoreType.DMA((2, len(SHARES))),
        ],
        compiler_params=pltpu.CompilerParams(
            collective_id=0, has_side_effects=True, vmem_limit_bytes=VMEM_FACTOR),
        name='factor',
    )(p_part, merged)
    err_new, p_o, qn_o = pl.pallas_call(
        error_kernel,
        out_shape=(jax.ShapeDtypeStruct((D_IN, D_OUT), F32), jax.ShapeDtypeStruct((RANK, D_IN), F32),
                   jax.ShapeDtypeStruct((RANK, D_OUT), F32)),
        in_specs=[vm, vm, vm],
        out_specs=(anyspec, vm, vm),
        scratch_shapes=[pltpu.VMEM((D_IN, D_OUT), F32), pltpu.VMEM((D_IN, 6 * RANK), BF16),
                        pltpu.VMEM((6 * RANK, D_OUT), BF16), pltpu.SemaphoreType.DMA((len(BANDS),))],
        compiler_params=pltpu.CompilerParams(vmem_limit_bytes=VMEM_ERROR),
        name='new_error',
    )(p_t, qn_t, merged)
    return p_o.T, qn_o.T, err_new[None]


def solution(mesh):
    return jax.shard_map(
        per_device, mesh=mesh,
        in_specs=(P('data', None), P('data', None), P('data', None), P(None, None), P('data', None, None)),
        out_specs=(P(None, None), P(None, None), P('data', None, None)), check_vma=False)
```

```python
import jax
import jax.numpy as jnp
from jax import lax
from jax.experimental import pallas as pl
from jax.experimental.pallas import tpu as pltpu
from jax.sharding import PartitionSpec as P

F32 = jnp.float32
BF16 = jnp.bfloat16
GROUP = 8
ROWS = 1024
D_IN = 896
D_OUT = 4864
RANK = 8
LANES = 128
CHUNK = 256
N_CHUNK = D_OUT // CHUNK
HALF = D_OUT // 2
SIDE = D_IN // 2
BANDS = ((0, 32), (32, 96), (128, 128), (256, 128), (384, 128), (512, 128), (640, 128), (768, 128))
SHARES = ((0, 512), (512, 512), (1024, 512), (1536, 512), (2048, 384))
SLAB = 64
SLABS = SIDE // SLAB
PADDED = 4 * RANK
AHEAD = 4
MESH = pl.DeviceIdType.MESH
C0 = 0.7978845608028654
C1 = 0.044715
VMEM_MERGE = 44 * 1024 * 1024
VMEM_FACTOR = 44 * 1024 * 1024
VMEM_ERROR = 24 * 1024 * 1024


def split3(x):
    hi = x.astype(BF16)
    rest = x - hi.astype(F32)
    mid = rest.astype(BF16)
    low = (rest - mid.astype(F32)).astype(BF16)
    return hi, mid, low


def stacked(parts):
    return jnp.concatenate([p.astype(F32) for p in parts], axis=0).astype(BF16)


def gelu_grad_times(z, dy):
    x = z.astype(F32)
    sq = x * x
    s = lax.logistic(x * (2.0 * C0 + (2.0 * C0 * C1) * sq))
    r = 2.0 * C0 + (6.0 * C0 * C1) * sq
    return (s * (1.0 + ((1.0 - s) * x) * r) * dy.astype(F32)).astype(BF16)


def orthonormal_rows(p0):
    p0 = p0 / jnp.max(jnp.abs(p0), axis=1, keepdims=True)
    row = lax.broadcasted_iota(jnp.int32, (RANK, 1), 0)
    cur = p0
    for k in range(RANK):
        v = jnp.broadcast_to(cur[k:k + 1, :], cur.shape)
        inv = lax.rsqrt(jnp.sum(v * v, axis=1, keepdims=True))
        coef = jnp.sum(v * p0, axis=1, keepdims=True) * inv
        q = v * inv
        cur = jnp.where(row == k, q, cur - jnp.where(row > k, coef, 0.0) * q)
    return cur


def wide(ref, first, rows):
    return jnp.concatenate([ref[first, rows, :], ref[first + 1, rows, :]], axis=1)


def merge_kernel(a_hbm, z_hbm, dy_hbm, qt_ref, e_hbm, m_ref, p_ref,
                 a_v, z_v, dy_v, at_ref, q3_v, g0, g1, pc0, pc1, sem_in, sem_a):
    gs = (g0, g1)
    pieces = (pc0, pc1)

    def cols_of(c):
        return pl.ds(c * CHUNK if isinstance(c, int) else pl.multiple_of(c * CHUNK, CHUNK), CHUNK)

    def copy(k, c):
        src, dst = ((z_hbm, z_v), (dy_hbm, dy_v), (e_hbm, m_ref))[k]
        return pltpu.make_async_copy(src.at[:, cols_of(c)], dst.at[:, cols_of(c)], sem_in.at[k, c])

    def start(c):
        for k in range(3):
            copy(k, c).start(priority=1)

    def gelu_slab(c, j):
        rows = pl.ds(j * SLAB, SLAB)
        g = gelu_grad_times(z_v[rows, cols_of(c)], dy_v[rows, cols_of(c)])
        for b in range(2):
            gs[c_par(c)][b, rows, :] = g[:, b * LANES:(b + 1) * LANES]

    par_box = [0]

    def c_par(c):
        return par_box[0] ^ 1

    def body_of(accs, p_acc):
        def merge_slab(c, par, q, i):
            rows = pl.ds(q * SIDE + i * SLAB, SLAB)
            m = pltpu.matmul_pop(accs[par][q][i]) * (1.0 / ROWS) + m_ref[rows, cols_of(c)]
            m_ref[rows, cols_of(c)] = m
            for t, piece in enumerate(split3(m)):
                for b in range(2):
                    pieces[par][t, b, rows, :] = piece[:, b * LANES:(b + 1) * LANES]

        def grad_step(par, q, k):
            pltpu.matmul_push_rhs(wide(gs[par], 0, pl.ds(k * CHUNK, CHUNK)), staging_register=0, mxu_index=q)
            for i in range(SLABS):
                lhs = wide(at_ref, 2 * k, pl.ds(q * SIDE + i * SLAB, SLAB))
                pltpu.matmul_acc_lhs(accs[par][q][i], lhs, load_staged_rhs=0 if i == 0 else None)

        def rank_step(q3, par, q, blk, t):
            rows = pl.ds(q * SIDE + blk * (SIDE - CHUNK), CHUNK)
            tile = jnp.concatenate([pieces[par][t, 0, rows, :], pieces[par][t, 1, rows, :]], axis=1)
            pltpu.matmul_push_rhs(tile, staging_register=1, mxu_index=q, transpose=True)
            pltpu.matmul_acc_lhs(p_acc[q][blk], q3, load_staged_rhs=1)

        def step(c, par, gelu, grad, merge, rank):
            par_box[0] = par
            if gelu:
                copy(0, c + 1).wait()
                copy(1, c + 1).wait()
            if merge:
                copy(2, c - 1).wait()
            if rank:
                q3 = jnp.concatenate([q3_v[2 * (c - 2)], q3_v[2 * (c - 2) + 1]], axis=1)
            tiles = [(blk, t) for blk in range(2) for t in range(3)]
            mxu = []
            for k in range(4):
                if grad:
                    mxu.append(lambda q, k=k: grad_step(par, q, k))
                for n, (blk, t) in enumerate(tiles):
                    if rank and n * 4 // len(tiles) == k:
                        mxu.append(lambda q, blk=blk, t=t: rank_step(q3, par, q, blk, t))
            n_gelu = ROWS // SLAB
            if merge:
                for s in range(SLABS):
                    merge_slab(c - 1, par ^ 1, 0, s)
                    merge_slab(c - 1, par ^ 1, 1, s)
            for s in range(SLABS):
                for n, op in enumerate(mxu):
                    if n * SLABS // len(mxu) == s:
                        op(0)
                        op(1)
                if gelu:
                    for j in range(n_gelu):
                        if j * SLABS // n_gelu == s:
                            gelu_slab(c + 1, j)

        load_a = pltpu.make_async_copy(a_hbm, a_v, sem_a)
        load_a.start()
        copy(0, 0).start()
        copy(1, 0).start()
        copy(2, 0).start(priority=1)
        for c in range(1, AHEAD):
            start(c)
        qt = qt_ref[...]
        q_all = stacked(split3(qt) + (jnp.zeros_like(qt),))
        for b in range(2 * N_CHUNK):
            q3_v[b] = q_all[:, b * LANES:(b + 1) * LANES]
        load_a.wait()
        copy(0, 0).wait()
        copy(1, 0).wait()
        par_box[0] = 1
        for b in range(ROWS // LANES):
            at_ref[b] = a_v[b * LANES:(b + 1) * LANES, :].T
            gelu_slab(0, 2 * b)
            gelu_slab(0, 2 * b + 1)
        start(AHEAD)
        step(0, 0, True, True, False, False)
        start(AHEAD + 1)
        step(1, 1, True, True, True, False)

        def pair(i, carry):
            for par in range(2):
                c = 2 * i + par

                @pl.when(c + AHEAD < N_CHUNK)
                def _():
                    start(c + AHEAD)

                @pl.when(c + 1 < N_CHUNK)
                def _():
                    step(c, par, True, True, True, True)
            return carry

        lax.fori_loop(1, N_CHUNK // 2, pair, 0)
        step(N_CHUNK - 1, 0, False, True, True, True)
        step(N_CHUNK, 1, False, False, True, True)
        step(N_CHUNK + 1, 0, False, False, False, True)
        skip = 2 * CHUNK - SIDE
        out = []
        for q in range(2):
            for blk in range(2):
                p3 = pltpu.matmul_pop(p_acc[q][blk])
                part = p3[0:8] + p3[8:16] + p3[16:24]
                out.append(part[:, skip:] if blk else part)
        p_ref[...] = jnp.concatenate(out, axis=1)

    def acc(q, rows):
        return pltpu.ACC(q)((rows, CHUNK), F32)

    pl.run_scoped(
        body_of,
        tuple(tuple(tuple(acc(q, SLAB) for _ in range(SLABS)) for q in range(2)) for _ in range(2)),
        tuple(tuple(acc(q, PADDED) for _ in range(2)) for q in range(2)))


def factor_kernel(p_in, m_in, pt_ref, qn_ref, m_ref, p_all, p3_v, pc_v, q_mine, q_part, q_pair, q_all,
                  sem_ps, sem_pr, sem_d, sem_is, sem_ir, sem_f):
    me = lax.axis_index('data')
    core = lax.rem(me, 2)
    chip = me // 2
    mate = me + 1 - 2 * core

    barrier = pltpu.get_barrier_semaphore()
    for d in range(1, GROUP):
        pl.semaphore_signal(barrier, inc=1, device_id=(lax.rem(me + d, GROUP),), device_id_type=MESH)
    p_all[me] = pt_ref[...]
    pl.semaphore_wait(barrier, GROUP - 1)

    def p_copy(d):
        return pltpu.make_async_remote_copy(
            src_ref=pt_ref, dst_ref=p_all.at[me], send_sem=sem_ps.at[d], recv_sem=sem_pr.at[d],
            device_id=(lax.rem(me + d, GROUP),), device_id_type=MESH)

    work = []
    for g, (off, width) in enumerate(SHARES):
        for mine in range(2):
            work.append((g, mine, off, width))

    def split_all():
        def one(b, carry):
            cols = pl.ds(pl.multiple_of(b * LANES, LANES), LANES)
            for r in range(0, D_IN, SLAB):
                rows = pl.ds(r, SLAB)
                for t, piece in enumerate(split3(m_ref[rows, cols])):
                    pc_v[t, b, rows, :] = piece
            return carry

        lax.fori_loop(0, D_OUT // LANES, one, 0)

    def rank_block(n):
        _, mine, off, width = work[n]
        half = core if mine else 1 - core
        first = half * (HALF // LANES) + off // LANES
        p3 = jnp.concatenate([p3_v[b] for b in range(D_IN // LANES)], axis=1)
        acc = None
        for t in range(3):
            tile = jnp.concatenate([pc_v[t, first + b] for b in range(width // LANES)], axis=1)
            part = jnp.dot(p3, tile, preferred_element_type=F32)
            acc = part if acc is None else acc + part
        dst = q_mine if mine else q_part
        dst[:, off:off + width] = acc[0:8] + acc[8:16] + acc[16:24]

    def to_mate(g):
        cols = pl.ds(*SHARES[g])
        return pltpu.make_async_remote_copy(
            src_ref=q_part.at[:, cols], dst_ref=q_pair.at[:, cols], send_sem=sem_d.at[0, g],
            recv_sem=sem_d.at[1, g], device_id=(mate,), device_id_type=MESH)

    def to_chip(g, d):
        view = q_all.at[chip, :, pl.ds(*SHARES[g])]
        return pltpu.make_async_remote_copy(
            src_ref=view, dst_ref=view, send_sem=sem_is.at[d, g], recv_sem=sem_ir.at[d, g],
            device_id=(lax.rem(me + 2 * d, GROUP),), device_id_type=MESH)

    def my_cols(g):
        off, width = SHARES[g]
        return pl.ds(pl.multiple_of(core * HALF + off, LANES), width)

    def final(g):
        view = qn_ref.at[:, my_cols(g)]
        return pltpu.make_async_remote_copy(
            src_ref=view, dst_ref=view, send_sem=sem_f.at[0, g], recv_sem=sem_f.at[1, g],
            device_id=(mate,), device_id_type=MESH)

    def share_chip_sum(g):
        cols = pl.ds(*SHARES[g])
        to_mate(g).wait()
        q_all[chip, :, cols] = q_mine[:, cols] + q_pair[:, cols]
        for d in (2, 1, 3):
            to_chip(g, d).start()

    for d in range(1, GROUP):
        p_copy(d).start()
    split_all()
    for d in range(1, GROUP):
        p_copy(d).wait()
    p_sum = p_all[0]
    for d in range(1, GROUP):
        p_sum = p_sum + p_all[d]
    p_t = orthonormal_rows(p_sum)
    pt_ref[...] = p_t
    p3 = stacked(split3(p_t) + (jnp.zeros_like(p_t),))
    for b in range(D_IN // LANES):
        p3_v[b] = p3[:, b * LANES:(b + 1) * LANES]

    for n, (g, mine, off, width) in enumerate(work):
        rank_block(n)
        last = n + 1 == len(work) or work[n + 1][:2] != (g, mine)
        if last and not mine:
            to_mate(g).start()
        if last and mine:
            if g:
                share_chip_sum(g - 1)
    share_chip_sum(len(SHARES) - 1)
    for g in range(len(SHARES)):
        cols = pl.ds(*SHARES[g])
        for d in range(1, 4):
            to_chip(g, d).wait()
        qn_ref[:, my_cols(g)] = (q_all[0, :, cols] + q_all[1, :, cols] + q_all[2, :, cols] + q_all[3, :, cols]) * (1.0 / GROUP)
        final(g).start()
    for g in range(len(SHARES)):
        final(g).wait()


def error_kernel(pt_ref, qn_ref, m_ref, e_hbm, po_ref, qo_ref, e_v, left_ref, right_ref, sem):
    po_ref[...] = pt_ref[...]
    qo_ref[...] = qn_ref[...]
    ph, pm, pl_ = split3(pt_ref[...])
    qh, qm, ql = split3(qn_ref[...])
    left_ref[...] = stacked((ph, ph, ph, pm, pm, pl_)).T
    right_ref[...] = stacked((qh, qm, ql, qh, qm, qh))

    def copy(n):
        rows = pl.ds(*BANDS[n])
        return pltpu.make_async_copy(e_v.at[rows, :], e_hbm.at[rows, :], sem.at[n])

    for n, band in enumerate(BANDS):
        rows = pl.ds(*band)
        e_v[rows, :] = m_ref[rows, :] - jnp.dot(left_ref[rows, :], right_ref[...], preferred_element_type=F32)
        copy(n).start()
    for n in range(len(BANDS)):
        copy(n).wait()


def per_device(act_in, pre_act, grad_out, q_init, err_mem):
    vm = pl.BlockSpec(memory_space=pltpu.VMEM)
    anyspec = pl.BlockSpec(memory_space=pl.ANY)
    merged, p_part = pl.pallas_call(
        merge_kernel,
        out_shape=(pltpu.VMEM((D_IN, D_OUT), F32), pltpu.VMEM((RANK, D_IN), F32)),
        in_specs=[anyspec, anyspec, anyspec, vm, anyspec],
        out_specs=(vm, vm),
        scratch_shapes=[
            pltpu.VMEM((ROWS, D_IN), BF16),
            pltpu.VMEM((ROWS, D_OUT), BF16),
            pltpu.VMEM((ROWS, D_OUT), BF16),
            pltpu.VMEM((ROWS // LANES, D_IN, LANES), BF16),
            pltpu.VMEM((2 * N_CHUNK, PADDED, LANES), BF16),
            pltpu.VMEM((2, ROWS, LANES), BF16),
            pltpu.VMEM((2, ROWS, LANES), BF16),
            pltpu.VMEM((3, 2, D_IN, LANES), BF16),
            pltpu.VMEM((3, 2, D_IN, LANES), BF16),
            pltpu.SemaphoreType.DMA((3, N_CHUNK)),
            pltpu.SemaphoreType.DMA,
        ],
        compiler_params=pltpu.CompilerParams(vmem_limit_bytes=VMEM_MERGE),
        name='merge',
    )(act_in, pre_act, grad_out, q_init.T, err_mem.reshape(D_IN, D_OUT))
    p_t, qn_t, merged = pl.pallas_call(
        factor_kernel,
        out_shape=(pltpu.VMEM((RANK, D_IN), F32), pltpu.VMEM((RANK, D_OUT), F32), pltpu.VMEM((D_IN, D_OUT), F32)),
        in_specs=[vm, vm],
        out_specs=(vm, vm, vm),
        input_output_aliases={0: 0, 1: 2},
        scratch_shapes=[
            pltpu.VMEM((GROUP, RANK, D_IN), F32),
            pltpu.VMEM((D_IN // LANES, PADDED, LANES), BF16),
            pltpu.VMEM((3, D_OUT // LANES, D_IN, LANES), BF16),
            pltpu.VMEM((RANK, HALF), F32),
            pltpu.VMEM((RANK, HALF), F32),
            pltpu.VMEM((RANK, HALF), F32),
            pltpu.VMEM((4, RANK, HALF), F32),
            pltpu.SemaphoreType.DMA((GROUP,)),
            pltpu.SemaphoreType.DMA((GROUP,)),
            pltpu.SemaphoreType.DMA((2, len(SHARES))),
            pltpu.SemaphoreType.DMA((4, len(SHARES))),
            pltpu.SemaphoreType.DMA((4, len(SHARES))),
            pltpu.SemaphoreType.DMA((2, len(SHARES))),
        ],
        compiler_params=pltpu.CompilerParams(
            collective_id=0, has_side_effects=True, vmem_limit_bytes=VMEM_FACTOR),
        name='factor',
    )(p_part, merged)
    err_new, p_o, qn_o = pl.pallas_call(
        error_kernel,
        out_shape=(jax.ShapeDtypeStruct((D_IN, D_OUT), F32), jax.ShapeDtypeStruct((RANK, D_IN), F32),
                   jax.ShapeDtypeStruct((RANK, D_OUT), F32)),
        in_specs=[vm, vm, vm],
        out_specs=(anyspec, vm, vm),
        scratch_shapes=[pltpu.VMEM((D_IN, D_OUT), F32), pltpu.VMEM((D_IN, 6 * RANK), BF16),
                        pltpu.VMEM((6 * RANK, D_OUT), BF16), pltpu.SemaphoreType.DMA((len(BANDS),))],
        compiler_params=pltpu.CompilerParams(vmem_limit_bytes=VMEM_ERROR),
        name='new_error',
    )(p_t, qn_t, merged)
    return p_o.T, qn_o.T, err_new[None]


def solution(mesh):
    return jax.shard_map(
        per_device, mesh=mesh,
        in_specs=(P('data', None), P('data', None), P('data', None), P(None, None), P('data', None, None)),
        out_specs=(P(None, None), P(None, None), P('data', None, None)), check_vma=False)
```

```python
import jax
import jax.numpy as jnp
from jax import lax
from jax.experimental import pallas as pl
from jax.experimental.pallas import tpu as pltpu
from jax.sharding import PartitionSpec as P

F32 = jnp.float32
BF16 = jnp.bfloat16
GROUP = 8
ROWS = 1024
D_IN = 896
D_OUT = 4864
RANK = 8
LANES = 128
CHUNK = 256
N_CHUNK = D_OUT // CHUNK
HALF = D_OUT // 2
SIDE = D_IN // 2
SHARES = ((0, 512), (512, 512), (1024, 512), (1536, 512), (2048, 384))
SLAB = 64
SLABS = SIDE // SLAB
PADDED = 4 * RANK
AHEAD = 4
MESH = pl.DeviceIdType.MESH
C0 = 0.7978845608028654
C1 = 0.044715
VMEM_MERGE = 44 * 1024 * 1024
VMEM_FACTOR = 44 * 1024 * 1024
VMEM_ERROR = 24 * 1024 * 1024


def split3(x):
    hi = x.astype(BF16)
    rest = x - hi.astype(F32)
    mid = rest.astype(BF16)
    low = (rest - mid.astype(F32)).astype(BF16)
    return hi, mid, low


def stacked(parts):
    return jnp.concatenate([p.astype(F32) for p in parts], axis=0).astype(BF16)


def gelu_grad_times(z, dy):
    x = z.astype(F32)
    sq = x * x
    s = lax.logistic(x * (2.0 * C0 + (2.0 * C0 * C1) * sq))
    r = 2.0 * C0 + (6.0 * C0 * C1) * sq
    return (s * (1.0 + ((1.0 - s) * x) * r) * dy.astype(F32)).astype(BF16)


def orthonormal_rows(p0):
    p0 = p0 / jnp.max(jnp.abs(p0), axis=1, keepdims=True)
    row = lax.broadcasted_iota(jnp.int32, (RANK, 1), 0)
    cur = p0
    for k in range(RANK):
        v = jnp.broadcast_to(cur[k:k + 1, :], cur.shape)
        inv = lax.rsqrt(jnp.sum(v * v, axis=1, keepdims=True))
        coef = jnp.sum(v * p0, axis=1, keepdims=True) * inv
        q = v * inv
        cur = jnp.where(row == k, q, cur - jnp.where(row > k, coef, 0.0) * q)
    return cur


def wide(ref, first, rows):
    return jnp.concatenate([ref[first, rows, :], ref[first + 1, rows, :]], axis=1)


def merge_kernel(a_hbm, z_hbm, dy_hbm, qt_ref, e_hbm, m_ref, p_ref,
                 a_v, z_v, dy_v, at_ref, q3_v, g0, g1, pc0, pc1, sem_in, sem_a):
    gs = (g0, g1)
    pieces = (pc0, pc1)

    def cols_of(c):
        return pl.ds(c * CHUNK if isinstance(c, int) else pl.multiple_of(c * CHUNK, CHUNK), CHUNK)

    def copy(k, c):
        src, dst = ((z_hbm, z_v), (dy_hbm, dy_v), (e_hbm, m_ref))[k]
        return pltpu.make_async_copy(src.at[:, cols_of(c)], dst.at[c], sem_in.at[k, c])

    def start(c):
        for k in range(3):
            copy(k, c).start(priority=1)

    def gelu_slab(c, j):
        rows = pl.ds(j * SLAB, SLAB)
        g = gelu_grad_times(z_v[c, rows, :], dy_v[c, rows, :])
        for b in range(2):
            gs[c_par(c)][b, rows, :] = g[:, b * LANES:(b + 1) * LANES]

    par_box = [0]

    def c_par(c):
        return par_box[0] ^ 1

    def body_of(accs, p_acc):
        def merge_slab(c, par, q, i):
            rows = pl.ds(q * SIDE + i * SLAB, SLAB)
            m = pltpu.matmul_pop(accs[par][q][i]) * (1.0 / ROWS) + m_ref[c, rows, :]
            m_ref[c, rows, :] = m
            for t, piece in enumerate(split3(m)):
                for b in range(2):
                    pieces[par][t, b, rows, :] = piece[:, b * LANES:(b + 1) * LANES]

        def grad_step(par, q, k):
            pltpu.matmul_push_rhs(wide(gs[par], 0, pl.ds(k * CHUNK, CHUNK)), staging_register=0, mxu_index=q)
            for i in range(SLABS):
                lhs = wide(at_ref, 2 * k, pl.ds(q * SIDE + i * SLAB, SLAB))
                pltpu.matmul_acc_lhs(accs[par][q][i], lhs, load_staged_rhs=0 if i == 0 else None)

        def rank_step(q3, par, q, blk, t):
            rows = pl.ds(q * SIDE + blk * (SIDE - CHUNK), CHUNK)
            tile = jnp.concatenate([pieces[par][t, 0, rows, :], pieces[par][t, 1, rows, :]], axis=1)
            pltpu.matmul_push_rhs(tile, staging_register=1, mxu_index=q, transpose=True)
            pltpu.matmul_acc_lhs(p_acc[q][blk], q3, load_staged_rhs=1)

        def step(c, par, gelu, grad, merge, rank):
            par_box[0] = par
            if gelu:
                copy(0, c + 1).wait()
                copy(1, c + 1).wait()
            if merge:
                copy(2, c - 1).wait()
            if rank:
                q3 = jnp.concatenate([q3_v[2 * (c - 2)], q3_v[2 * (c - 2) + 1]], axis=1)
            tiles = [(blk, t) for blk in range(2) for t in range(3)]
            mxu = []
            for k in range(4):
                if grad:
                    mxu.append(lambda q, k=k: grad_step(par, q, k))
                for n, (blk, t) in enumerate(tiles):
                    if rank and n * 4 // len(tiles) == k:
                        mxu.append(lambda q, blk=blk, t=t: rank_step(q3, par, q, blk, t))
            n_gelu = ROWS // SLAB
            if merge:
                for s in range(SLABS):
                    merge_slab(c - 1, par ^ 1, 0, s)
                    merge_slab(c - 1, par ^ 1, 1, s)
            for s in range(SLABS):
                for n, op in enumerate(mxu):
                    if n * SLABS // len(mxu) == s:
                        op(0)
                        op(1)
                if gelu:
                    for j in range(n_gelu):
                        if j * SLABS // n_gelu == s:
                            gelu_slab(c + 1, j)

        load_a = pltpu.make_async_copy(a_hbm, a_v, sem_a)
        load_a.start()
        copy(0, 0).start()
        copy(1, 0).start()
        copy(2, 0).start(priority=1)
        for c in range(1, AHEAD):
            start(c)
        qt = qt_ref[...]
        q_all = stacked(split3(qt) + (jnp.zeros_like(qt),))
        for b in range(2 * N_CHUNK):
            q3_v[b] = q_all[:, b * LANES:(b + 1) * LANES]
        load_a.wait()
        copy(0, 0).wait()
        copy(1, 0).wait()
        par_box[0] = 1
        for b in range(ROWS // LANES):
            at_ref[b] = a_v[b * LANES:(b + 1) * LANES, :].T
            gelu_slab(0, 2 * b)
            gelu_slab(0, 2 * b + 1)
        start(AHEAD)
        step(0, 0, True, True, False, False)
        start(AHEAD + 1)
        step(1, 1, True, True, True, False)

        def pair(i, carry):
            for par in range(2):
                c = 2 * i + par

                @pl.when(c + AHEAD < N_CHUNK)
                def _():
                    start(c + AHEAD)

                @pl.when(c + 1 < N_CHUNK)
                def _():
                    step(c, par, True, True, True, True)
            return carry

        lax.fori_loop(1, N_CHUNK // 2, pair, 0)
        step(N_CHUNK - 1, 0, False, True, True, True)
        step(N_CHUNK, 1, False, False, True, True)
        step(N_CHUNK + 1, 0, False, False, False, True)
        skip = 2 * CHUNK - SIDE
        out = []
        for q in range(2):
            for blk in range(2):
                p3 = pltpu.matmul_pop(p_acc[q][blk])
                part = p3[0:8] + p3[8:16] + p3[16:24]
                out.append(part[:, skip:] if blk else part)
        p_ref[...] = jnp.concatenate(out, axis=1)

    def acc(q, rows):
        return pltpu.ACC(q)((rows, CHUNK), F32)

    pl.run_scoped(
        body_of,
        tuple(tuple(tuple(acc(q, SLAB) for _ in range(SLABS)) for q in range(2)) for _ in range(2)),
        tuple(tuple(acc(q, PADDED) for _ in range(2)) for q in range(2)))


def factor_kernel(p_in, m_in, pt_ref, qn_ref, m_ref, p_all, p3_v, pc_v, q_mine, q_part, q_pair, q_all,
                  sem_ps, sem_pr, sem_d, sem_is, sem_ir, sem_f):
    me = lax.axis_index('data')
    core = lax.rem(me, 2)
    chip = me // 2
    mate = me + 1 - 2 * core

    barrier = pltpu.get_barrier_semaphore()
    for d in range(1, GROUP):
        pl.semaphore_signal(barrier, inc=1, device_id=(lax.rem(me + d, GROUP),), device_id_type=MESH)
    p_all[me] = p_in[...]
    pl.semaphore_wait(barrier, GROUP - 1)

    def p_copy(d):
        return pltpu.make_async_remote_copy(
            src_ref=p_in, dst_ref=p_all.at[me], send_sem=sem_ps.at[d], recv_sem=sem_pr.at[d],
            device_id=(lax.rem(me + d, GROUP),), device_id_type=MESH)

    work = []
    for g, (off, width) in enumerate(SHARES):
        for mine in range(2):
            work.append((g, mine, off, width))

    def split_all():
        def one(c, carry):
            for r in range(0, D_IN, SLAB):
                rows = pl.ds(r, SLAB)
                for t, piece in enumerate(split3(m_in[c, rows, :])):
                    for b in range(2):
                        pc_v[t, 2 * c + b, rows, :] = piece[:, b * LANES:(b + 1) * LANES]
            return carry

        lax.fori_loop(0, N_CHUNK, one, 0)

    def rank_block(n):
        _, mine, off, width = work[n]
        half = core if mine else 1 - core
        first = half * (HALF // LANES) + off // LANES
        p3 = jnp.concatenate([p3_v[b] for b in range(D_IN // LANES)], axis=1)
        acc = None
        for t in range(3):
            tile = jnp.concatenate([pc_v[t, first + b] for b in range(width // LANES)], axis=1)
            part = jnp.dot(p3, tile, preferred_element_type=F32)
            acc = part if acc is None else acc + part
        dst = q_mine if mine else q_part
        dst[:, off:off + width] = acc[0:8] + acc[8:16] + acc[16:24]

    def to_mate(g):
        cols = pl.ds(*SHARES[g])
        return pltpu.make_async_remote_copy(
            src_ref=q_part.at[:, cols], dst_ref=q_pair.at[:, cols], send_sem=sem_d.at[0, g],
            recv_sem=sem_d.at[1, g], device_id=(mate,), device_id_type=MESH)

    def to_chip(g, d):
        view = q_all.at[chip, :, pl.ds(*SHARES[g])]
        return pltpu.make_async_remote_copy(
            src_ref=view, dst_ref=view, send_sem=sem_is.at[d, g], recv_sem=sem_ir.at[d, g],
            device_id=(lax.rem(me + 2 * d, GROUP),), device_id_type=MESH)

    def my_cols(g):
        off, width = SHARES[g]
        return pl.ds(pl.multiple_of(core * HALF + off, LANES), width)

    def final(g):
        view = qn_ref.at[:, my_cols(g)]
        return pltpu.make_async_remote_copy(
            src_ref=view, dst_ref=view, send_sem=sem_f.at[0, g], recv_sem=sem_f.at[1, g],
            device_id=(mate,), device_id_type=MESH)

    def share_chip_sum(g):
        cols = pl.ds(*SHARES[g])
        to_mate(g).wait()
        q_all[chip, :, cols] = q_mine[:, cols] + q_pair[:, cols]
        for d in (2, 1, 3):
            to_chip(g, d).start()

    for d in range(1, GROUP):
        p_copy(d).start()
    split_all()
    for d in range(1, GROUP):
        p_copy(d).wait()
    p_sum = p_all[0]
    for d in range(1, GROUP):
        p_sum = p_sum + p_all[d]
    p_t = orthonormal_rows(p_sum)
    pt_ref[...] = p_t
    p3 = stacked(split3(p_t) + (jnp.zeros_like(p_t),))
    for b in range(D_IN // LANES):
        p3_v[b] = p3[:, b * LANES:(b + 1) * LANES]

    for n, (g, mine, off, width) in enumerate(work):
        rank_block(n)
        last = n + 1 == len(work) or work[n + 1][:2] != (g, mine)
        if last and not mine:
            to_mate(g).start()
        if last and mine:
            if g:
                share_chip_sum(g - 1)
    share_chip_sum(len(SHARES) - 1)
    for g in range(len(SHARES)):
        cols = pl.ds(*SHARES[g])
        for d in range(1, 4):
            to_chip(g, d).wait()
        qn_ref[:, my_cols(g)] = (q_all[0, :, cols] + q_all[1, :, cols] + q_all[2, :, cols] + q_all[3, :, cols]) * (1.0 / GROUP)
        final(g).start()
    for g in range(len(SHARES)):
        final(g).wait()


def error_kernel(pt_ref, qn_ref, m_ref, e_hbm, po_ref, qo_ref, e_v, left_ref, right_ref, sem):
    po_ref[...] = pt_ref[...]
    qo_ref[...] = qn_ref[...]
    ph, pm, pl_ = split3(pt_ref[...])
    qh, qm, ql = split3(qn_ref[...])
    left_ref[...] = stacked((ph, ph, ph, pm, pm, pl_)).T
    right_ref[...] = stacked((qh, qm, ql, qh, qm, qh))

    def copy(c):
        return pltpu.make_async_copy(e_v.at[c], e_hbm.at[:, pl.ds(c * CHUNK, CHUNK)], sem.at[c])

    for c in range(N_CHUNK):
        right = right_ref[:, c * CHUNK:(c + 1) * CHUNK]
        for r in range(0, D_IN, 224):
            rows = pl.ds(r, 224)
            e_v[c, rows, :] = m_ref[c, rows, :] - jnp.dot(left_ref[rows, :], right, preferred_element_type=F32)
        copy(c).start()
    for c in range(N_CHUNK):
        copy(c).wait()


def per_device(act_in, pre_act, grad_out, q_init, err_mem):
    vm = pl.BlockSpec(memory_space=pltpu.VMEM)
    anyspec = pl.BlockSpec(memory_space=pl.ANY)
    merged, p_part = pl.pallas_call(
        merge_kernel,
        out_shape=(pltpu.VMEM((N_CHUNK, D_IN, CHUNK), F32), pltpu.VMEM((RANK, D_IN), F32)),
        in_specs=[anyspec, anyspec, anyspec, vm, anyspec],
        out_specs=(vm, vm),
        scratch_shapes=[
            pltpu.VMEM((ROWS, D_IN), BF16),
            pltpu.VMEM((N_CHUNK, ROWS, CHUNK), BF16),
            pltpu.VMEM((N_CHUNK, ROWS, CHUNK), BF16),
            pltpu.VMEM((ROWS // LANES, D_IN, LANES), BF16),
            pltpu.VMEM((2 * N_CHUNK, PADDED, LANES), BF16),
            pltpu.VMEM((2, ROWS, LANES), BF16),
            pltpu.VMEM((2, ROWS, LANES), BF16),
            pltpu.VMEM((3, 2, D_IN, LANES), BF16),
            pltpu.VMEM((3, 2, D_IN, LANES), BF16),
            pltpu.SemaphoreType.DMA((3, N_CHUNK)),
            pltpu.SemaphoreType.DMA,
        ],
        compiler_params=pltpu.CompilerParams(vmem_limit_bytes=VMEM_MERGE),
        name='merge',
    )(act_in, pre_act, grad_out, q_init.T, err_mem.reshape(D_IN, D_OUT))
    p_t, qn_t, merged = pl.pallas_call(
        factor_kernel,
        out_shape=(pltpu.VMEM((RANK, D_IN), F32), pltpu.VMEM((RANK, D_OUT), F32), pltpu.VMEM((N_CHUNK, D_IN, CHUNK), F32)),
        in_specs=[vm, vm],
        out_specs=(vm, vm, vm),
        input_output_aliases={0: 0, 1: 2},
        scratch_shapes=[
            pltpu.VMEM((GROUP, RANK, D_IN), F32),
            pltpu.VMEM((D_IN // LANES, PADDED, LANES), BF16),
            pltpu.VMEM((3, D_OUT // LANES, D_IN, LANES), BF16),
            pltpu.VMEM((RANK, HALF), F32),
            pltpu.VMEM((RANK, HALF), F32),
            pltpu.VMEM((RANK, HALF), F32),
            pltpu.VMEM((4, RANK, HALF), F32),
            pltpu.SemaphoreType.DMA((GROUP,)),
            pltpu.SemaphoreType.DMA((GROUP,)),
            pltpu.SemaphoreType.DMA((2, len(SHARES))),
            pltpu.SemaphoreType.DMA((4, len(SHARES))),
            pltpu.SemaphoreType.DMA((4, len(SHARES))),
            pltpu.SemaphoreType.DMA((2, len(SHARES))),
        ],
        compiler_params=pltpu.CompilerParams(
            collective_id=0, has_side_effects=True, vmem_limit_bytes=VMEM_FACTOR),
        name='factor',
    )(p_part, merged)
    err_new, p_o, qn_o = pl.pallas_call(
        error_kernel,
        out_shape=(jax.ShapeDtypeStruct((D_IN, D_OUT), F32), jax.ShapeDtypeStruct((RANK, D_IN), F32),
                   jax.ShapeDtypeStruct((RANK, D_OUT), F32)),
        in_specs=[vm, vm, vm],
        out_specs=(anyspec, vm, vm),
        scratch_shapes=[pltpu.VMEM((N_CHUNK, D_IN, CHUNK), F32), pltpu.VMEM((D_IN, 6 * RANK), BF16),
                        pltpu.VMEM((6 * RANK, D_OUT), BF16), pltpu.SemaphoreType.DMA((N_CHUNK,))],
        compiler_params=pltpu.CompilerParams(vmem_limit_bytes=VMEM_ERROR),
        name='new_error',
    )(p_t, qn_t, merged)
    return p_o.T, qn_o.T, err_new[None]


def solution(mesh):
    return jax.shard_map(
        per_device, mesh=mesh,
        in_specs=(P('data', None), P('data', None), P('data', None), P(None, None), P('data', None, None)),
        out_specs=(P(None, None), P(None, None), P('data', None, None)), check_vma=False)
```

```python
import jax
import jax.numpy as jnp
from jax import lax
from jax.experimental import pallas as pl
from jax.experimental.pallas import tpu as pltpu
from jax.sharding import PartitionSpec as P

F32 = jnp.float32
BF16 = jnp.bfloat16
GROUP = 8
ROWS = 1024
D_IN = 896
D_OUT = 4864
RANK = 8
LANES = 128
CHUNK = 256
N_CHUNK = D_OUT // CHUNK
HALF = D_OUT // 2
SIDE = D_IN // 2
SHARES = ((0, 512), (512, 512), (1024, 512), (1536, 512), (2048, 256), (2304, 128))
LAST = len(SHARES) - 1
SLAB = 64
SLABS = SIDE // SLAB
PADDED = 4 * RANK
AHEAD = 4
MESH = pl.DeviceIdType.MESH
C0 = 0.7978845608028654
C1 = 0.044715
VMEM_MERGE = 44 * 1024 * 1024
VMEM_FACTOR = 44 * 1024 * 1024
VMEM_ERROR = 24 * 1024 * 1024


def split3(x):
    hi = x.astype(BF16)
    rest = x - hi.astype(F32)
    mid = rest.astype(BF16)
    low = (rest - mid.astype(F32)).astype(BF16)
    return hi, mid, low


def stacked(parts):
    return jnp.concatenate([p.astype(F32) for p in parts], axis=0).astype(BF16)


def gelu_grad_times(z, dy):
    x = z.astype(F32)
    sq = x * x
    s = lax.logistic(x * (2.0 * C0 + (2.0 * C0 * C1) * sq))
    r = 2.0 * C0 + (6.0 * C0 * C1) * sq
    return (s * (1.0 + ((1.0 - s) * x) * r) * dy.astype(F32)).astype(BF16)


def orthonormal_rows(p0):
    p0 = p0 / jnp.max(jnp.abs(p0), axis=1, keepdims=True)
    row = lax.broadcasted_iota(jnp.int32, (RANK, 1), 0)
    cur = p0
    for k in range(RANK):
        v = jnp.broadcast_to(cur[k:k + 1, :], cur.shape)
        inv = lax.rsqrt(jnp.sum(v * v, axis=1, keepdims=True))
        coef = jnp.sum(v * p0, axis=1, keepdims=True) * inv
        q = v * inv
        cur = jnp.where(row == k, q, cur - jnp.where(row > k, coef, 0.0) * q)
    return cur


def wide(ref, first, rows):
    return jnp.concatenate([ref[first, rows, :], ref[first + 1, rows, :]], axis=1)


def merge_kernel(a_hbm, z_hbm, dy_hbm, qt_hbm, e_hbm, m_ref, p_ref,
                 a_v, z_v, dy_v, qt_v, at_ref, q3_v, g0, g1, pc0, pc1, sem_in, sem_a, sem_q):
    gs = (g0, g1)
    pieces = (pc0, pc1)

    def cols_of(c):
        return pl.ds(c * CHUNK if isinstance(c, int) else pl.multiple_of(c * CHUNK, CHUNK), CHUNK)

    def copy(k, c):
        src, dst = ((z_hbm, z_v), (dy_hbm, dy_v), (e_hbm, m_ref))[k]
        return pltpu.make_async_copy(src.at[:, cols_of(c)], dst.at[c], sem_in.at[k, c])

    def start(c):
        for k in range(3):
            copy(k, c).start(priority=1)

    def gelu_slab(c, j):
        rows = pl.ds(j * SLAB, SLAB)
        g = gelu_grad_times(z_v[c, rows, :], dy_v[c, rows, :])
        for b in range(2):
            gs[c_par(c)][b, rows, :] = g[:, b * LANES:(b + 1) * LANES]

    par_box = [0]

    def c_par(c):
        return par_box[0] ^ 1

    def body_of(accs, p_acc):
        def merge_slab(c, par, q, i):
            rows = pl.ds(q * SIDE + i * SLAB, SLAB)
            m = pltpu.matmul_pop(accs[par][q][i]) * (1.0 / ROWS) + m_ref[c, rows, :]
            m_ref[c, rows, :] = m
            for t, piece in enumerate(split3(m)):
                for b in range(2):
                    pieces[par][t, b, rows, :] = piece[:, b * LANES:(b + 1) * LANES]

        def grad_step(par, q, k):
            pltpu.matmul_push_rhs(wide(gs[par], 0, pl.ds(k * CHUNK, CHUNK)), staging_register=0, mxu_index=q)
            for i in range(SLABS):
                lhs = wide(at_ref, 2 * k, pl.ds(q * SIDE + i * SLAB, SLAB))
                pltpu.matmul_acc_lhs(accs[par][q][i], lhs, load_staged_rhs=0 if i == 0 else None)

        def rank_step(q3, par, q, blk, t):
            rows = pl.ds(q * SIDE + blk * (SIDE - CHUNK), CHUNK)
            tile = jnp.concatenate([pieces[par][t, 0, rows, :], pieces[par][t, 1, rows, :]], axis=1)
            pltpu.matmul_push_rhs(tile, staging_register=1, mxu_index=q, transpose=True)
            pltpu.matmul_acc_lhs(p_acc[q][blk], q3, load_staged_rhs=1)

        def step(c, par, gelu, grad, merge, rank):
            par_box[0] = par
            if gelu:
                copy(0, c + 1).wait()
                copy(1, c + 1).wait()
            if merge:
                copy(2, c - 1).wait()
            if rank:
                q3 = jnp.concatenate([q3_v[2 * (c - 2)], q3_v[2 * (c - 2) + 1]], axis=1)
            tiles = [(blk, t) for blk in range(2) for t in range(3)]
            mxu = []
            for k in range(4):
                if grad:
                    mxu.append(lambda q, k=k: grad_step(par, q, k))
                for n, (blk, t) in enumerate(tiles):
                    if rank and n * 4 // len(tiles) == k:
                        mxu.append(lambda q, blk=blk, t=t: rank_step(q3, par, q, blk, t))
            n_gelu = ROWS // SLAB
            if merge:
                for s in range(SLABS):
                    merge_slab(c - 1, par ^ 1, 0, s)
                    merge_slab(c - 1, par ^ 1, 1, s)
            for s in range(SLABS):
                for n, op in enumerate(mxu):
                    if n * SLABS // len(mxu) == s:
                        op(0)
                        op(1)
                if gelu:
                    for j in range(n_gelu):
                        if j * SLABS // n_gelu == s:
                            gelu_slab(c + 1, j)

        load_a = pltpu.make_async_copy(a_hbm, a_v, sem_a)
        load_a.start()
        copy(0, 0).start()
        copy(1, 0).start()
        load_q = pltpu.make_async_copy(qt_hbm, qt_v, sem_q)
        load_q.start(priority=1)
        copy(2, 0).start(priority=1)
        for c in range(1, AHEAD):
            start(c)
        load_a.wait()
        copy(0, 0).wait()
        copy(1, 0).wait()
        par_box[0] = 1
        for b in range(ROWS // LANES):
            at_ref[b] = a_v[b * LANES:(b + 1) * LANES, :].T
            gelu_slab(0, 2 * b)
            gelu_slab(0, 2 * b + 1)
        start(AHEAD)
        load_q.wait()
        qt = qt_v[...]
        q_all = stacked(split3(qt) + (jnp.zeros_like(qt),))
        for b in range(2 * N_CHUNK):
            q3_v[b] = q_all[:, b * LANES:(b + 1) * LANES]
        step(0, 0, True, True, False, False)
        start(AHEAD + 1)
        step(1, 1, True, True, True, False)

        def pair(i, carry):
            for par in range(2):
                c = 2 * i + par

                @pl.when(c + AHEAD < N_CHUNK)
                def _():
                    start(c + AHEAD)

                @pl.when(c + 1 < N_CHUNK)
                def _():
                    step(c, par, True, True, True, True)
            return carry

        lax.fori_loop(1, N_CHUNK // 2, pair, 0)
        step(N_CHUNK - 1, 0, False, True, True, True)
        step(N_CHUNK, 1, False, False, True, True)
        step(N_CHUNK + 1, 0, False, False, False, True)
        skip = 2 * CHUNK - SIDE
        out = []
        for q in range(2):
            for blk in range(2):
                p3 = pltpu.matmul_pop(p_acc[q][blk])
                part = p3[0:8] + p3[8:16] + p3[16:24]
                out.append(part[:, skip:] if blk else part)
        p_ref[...] = jnp.concatenate(out, axis=1)

    def acc(q, rows):
        return pltpu.ACC(q)((rows, CHUNK), F32)

    pl.run_scoped(
        body_of,
        tuple(tuple(tuple(acc(q, SLAB) for _ in range(SLABS)) for q in range(2)) for _ in range(2)),
        tuple(tuple(acc(q, PADDED) for _ in range(2)) for q in range(2)))


def factor_kernel(p_in, m_in, pt_ref, qn_ref, m_ref, p_all, p3_v, pc_v, q_mine, q_part, q_pair, q_all, q_other,
                  sem_ps, sem_pr, sem_d, sem_is, sem_ir, sem_f, sem_o):
    me = lax.axis_index('data')
    core = lax.rem(me, 2)
    chip = me // 2
    mate = me + 1 - 2 * core

    barrier = pltpu.get_barrier_semaphore()
    for d in range(1, GROUP):
        pl.semaphore_signal(barrier, inc=1, device_id=(lax.rem(me + d, GROUP),), device_id_type=MESH)
    p_all[me] = p_in[...]
    pl.semaphore_wait(barrier, GROUP - 1)

    def p_copy(d):
        return pltpu.make_async_remote_copy(
            src_ref=p_in, dst_ref=p_all.at[me], send_sem=sem_ps.at[d], recv_sem=sem_pr.at[d],
            device_id=(lax.rem(me + d, GROUP),), device_id_type=MESH)

    work = [(0, 0)]
    for g in range(LAST):
        work += [(g + 1, 0), (g, 1)]
    work.append((LAST, 1))

    def split_all():
        def one(c, carry):
            for r in range(0, D_IN, SLAB):
                rows = pl.ds(r, SLAB)
                for t, piece in enumerate(split3(m_in[c, rows, :])):
                    for b in range(2):
                        pc_v[t, 2 * c + b, rows, :] = piece[:, b * LANES:(b + 1) * LANES]
            return carry

        lax.fori_loop(0, N_CHUNK, one, 0)

    def rank_block(n):
        g, mine = work[n]
        off, width = SHARES[g]
        half = core if mine else 1 - core
        first = half * (HALF // LANES) + off // LANES
        p3 = jnp.concatenate([p3_v[b] for b in range(D_IN // LANES)], axis=1)
        acc = None
        for t in range(3):
            tile = jnp.concatenate([pc_v[t, first + b] for b in range(width // LANES)], axis=1)
            part = jnp.dot(p3, tile, preferred_element_type=F32)
            acc = part if acc is None else acc + part
        dst = q_mine if mine else q_part
        dst[:, off:off + width] = acc[0:8] + acc[8:16] + acc[16:24]

    def to_mate(g):
        cols = pl.ds(*SHARES[g])
        return pltpu.make_async_remote_copy(
            src_ref=q_part.at[:, cols], dst_ref=q_pair.at[:, cols], send_sem=sem_d.at[0, g],
            recv_sem=sem_d.at[1, g], device_id=(mate,), device_id_type=MESH)

    def to_chip(g, d):
        view = q_all.at[chip, :, pl.ds(*SHARES[g])]
        return pltpu.make_async_remote_copy(
            src_ref=view, dst_ref=view, send_sem=sem_is.at[d, g], recv_sem=sem_ir.at[d, g],
            device_id=(lax.rem(me + 2 * d, GROUP),), device_id_type=MESH)

    def my_cols(g):
        off, width = SHARES[g]
        return pl.ds(pl.multiple_of(core * HALF + off, LANES), width)

    def final(g):
        view = qn_ref.at[:, my_cols(g)]
        return pltpu.make_async_remote_copy(
            src_ref=view, dst_ref=view, send_sem=sem_f.at[0, g], recv_sem=sem_f.at[1, g],
            device_id=(mate,), device_id_type=MESH)

    def to_other(d):
        return pltpu.make_async_remote_copy(
            src_ref=q_all.at[chip, :, pl.ds(*SHARES[LAST])], dst_ref=q_other.at[chip], send_sem=sem_o.at[0, d],
            recv_sem=sem_o.at[1, d], device_id=(lax.rem(mate + 2 * d, GROUP),), device_id_type=MESH)

    mate_cols = pl.ds(pl.multiple_of((1 - core) * HALF + SHARES[LAST][0], LANES), SHARES[LAST][1])

    def mean_of(parts):
        return (parts[0] + parts[1] + parts[2] + parts[3]) * (1.0 / GROUP)

    def share_chip_sum(g):
        cols = pl.ds(*SHARES[g])
        to_mate(g).wait()
        q_all[chip, :, cols] = q_mine[:, cols] + q_pair[:, cols]
        for d in (2, 1, 3):
            to_chip(g, d).start()
            if g == LAST:
                to_other(d).start()
        if g == LAST:
            to_other(0).start()

    for d in range(1, GROUP):
        p_copy(d).start()
    split_all()
    for d in range(1, GROUP):
        p_copy(d).wait()
    p_sum = p_all[0]
    for d in range(1, GROUP):
        p_sum = p_sum + p_all[d]
    p_t = orthonormal_rows(p_sum)
    pt_ref[...] = p_t
    p3 = stacked(split3(p_t) + (jnp.zeros_like(p_t),))
    for b in range(D_IN // LANES):
        p3_v[b] = p3[:, b * LANES:(b + 1) * LANES]

    for n, (g, mine) in enumerate(work):
        rank_block(n)
        if mine:
            share_chip_sum(g)
        else:
            to_mate(g).start()
    for g in range(len(SHARES)):
        cols = pl.ds(*SHARES[g])
        for d in range(1, 4):
            to_chip(g, d).wait()
        qn_ref[:, my_cols(g)] = mean_of([q_all[k, :, cols] for k in range(4)])
        if g < LAST:
            final(g).start()
    for d in range(4):
        to_other(d).wait()
    qn_ref[:, mate_cols] = mean_of([q_other[k] for k in range(4)])
    for g in range(LAST):
        final(g).wait()


def error_kernel(pt_ref, qn_ref, m_ref, e_hbm, po_hbm, qo_hbm, e_v, left_ref, right_ref, sem):
    factors = (pltpu.make_async_copy(pt_ref, po_hbm, sem.at[N_CHUNK]),
               pltpu.make_async_copy(qn_ref, qo_hbm, sem.at[N_CHUNK + 1]))
    for move in factors:
        move.start()
    ph, pm, pl_ = split3(pt_ref[...])
    qh, qm, ql = split3(qn_ref[...])
    left_ref[...] = stacked((ph, ph, ph, pm, pm, pl_)).T
    right_ref[...] = stacked((qh, qm, ql, qh, qm, qh))

    def copy(c):
        return pltpu.make_async_copy(e_v.at[c], e_hbm.at[:, pl.ds(c * CHUNK, CHUNK)], sem.at[c])

    for c in range(N_CHUNK):
        right = right_ref[:, c * CHUNK:(c + 1) * CHUNK]
        for r in range(0, D_IN, 224):
            rows = pl.ds(r, 224)
            e_v[c, rows, :] = m_ref[c, rows, :] - jnp.dot(left_ref[rows, :], right, preferred_element_type=F32)
        copy(c).start()
    for move in factors:
        move.wait()
    for c in range(N_CHUNK):
        copy(c).wait()


def per_device(act_in, pre_act, grad_out, q_init, err_mem):
    vm = pl.BlockSpec(memory_space=pltpu.VMEM)
    anyspec = pl.BlockSpec(memory_space=pl.ANY)
    merged, p_part = pl.pallas_call(
        merge_kernel,
        out_shape=(pltpu.VMEM((N_CHUNK, D_IN, CHUNK), F32), pltpu.VMEM((RANK, D_IN), F32)),
        in_specs=[anyspec, anyspec, anyspec, anyspec, anyspec],
        out_specs=(vm, vm),
        scratch_shapes=[
            pltpu.VMEM((ROWS, D_IN), BF16),
            pltpu.VMEM((N_CHUNK, ROWS, CHUNK), BF16),
            pltpu.VMEM((N_CHUNK, ROWS, CHUNK), BF16),
            pltpu.VMEM((RANK, D_OUT), F32),
            pltpu.VMEM((ROWS // LANES, D_IN, LANES), BF16),
            pltpu.VMEM((2 * N_CHUNK, PADDED, LANES), BF16),
            pltpu.VMEM((2, ROWS, LANES), BF16),
            pltpu.VMEM((2, ROWS, LANES), BF16),
            pltpu.VMEM((3, 2, D_IN, LANES), BF16),
            pltpu.VMEM((3, 2, D_IN, LANES), BF16),
            pltpu.SemaphoreType.DMA((3, N_CHUNK)),
            pltpu.SemaphoreType.DMA,
            pltpu.SemaphoreType.DMA,
        ],
        compiler_params=pltpu.CompilerParams(vmem_limit_bytes=VMEM_MERGE),
        name='merge',
    )(act_in, pre_act, grad_out, q_init.T, err_mem.reshape(D_IN, D_OUT))
    p_t, qn_t, merged = pl.pallas_call(
        factor_kernel,
        out_shape=(pltpu.VMEM((RANK, D_IN), F32), pltpu.VMEM((RANK, D_OUT), F32), pltpu.VMEM((N_CHUNK, D_IN, CHUNK), F32)),
        in_specs=[vm, vm],
        out_specs=(vm, vm, vm),
        input_output_aliases={0: 0, 1: 2},
        scratch_shapes=[
            pltpu.VMEM((GROUP, RANK, D_IN), F32),
            pltpu.VMEM((D_IN // LANES, PADDED, LANES), BF16),
            pltpu.VMEM((3, D_OUT // LANES, D_IN, LANES), BF16),
            pltpu.VMEM((RANK, HALF), F32),
            pltpu.VMEM((RANK, HALF), F32),
            pltpu.VMEM((RANK, HALF), F32),
            pltpu.VMEM((4, RANK, HALF), F32),
            pltpu.VMEM((4, RANK, SHARES[LAST][1]), F32),
            pltpu.SemaphoreType.DMA((GROUP,)),
            pltpu.SemaphoreType.DMA((GROUP,)),
            pltpu.SemaphoreType.DMA((2, len(SHARES))),
            pltpu.SemaphoreType.DMA((4, len(SHARES))),
            pltpu.SemaphoreType.DMA((4, len(SHARES))),
            pltpu.SemaphoreType.DMA((2, len(SHARES))),
            pltpu.SemaphoreType.DMA((2, 4)),
        ],
        compiler_params=pltpu.CompilerParams(
            collective_id=0, has_side_effects=True, vmem_limit_bytes=VMEM_FACTOR),
        name='factor',
    )(p_part, merged)
    err_new, p_o, qn_o = pl.pallas_call(
        error_kernel,
        out_shape=(jax.ShapeDtypeStruct((D_IN, D_OUT), F32), jax.ShapeDtypeStruct((RANK, D_IN), F32),
                   jax.ShapeDtypeStruct((RANK, D_OUT), F32)),
        in_specs=[vm, vm, vm],
        out_specs=(anyspec, anyspec, anyspec),
        scratch_shapes=[pltpu.VMEM((N_CHUNK, D_IN, CHUNK), F32), pltpu.VMEM((D_IN, 6 * RANK), BF16),
                        pltpu.VMEM((6 * RANK, D_OUT), BF16), pltpu.SemaphoreType.DMA((N_CHUNK + 2,))],
        compiler_params=pltpu.CompilerParams(vmem_limit_bytes=VMEM_ERROR),
        name='new_error',
    )(p_t, qn_t, merged)
    return p_o.T, qn_o.T, err_new[None]


def solution(mesh):
    return jax.shard_map(
        per_device, mesh=mesh,
        in_specs=(P('data', None), P('data', None), P('data', None), P(None, None), P('data', None, None)),
        out_specs=(P(None, None), P(None, None), P('data', None, None)), check_vma=False)
```

```python
import jax
import jax.numpy as jnp
from jax import lax
from jax.experimental import pallas as pl
from jax.experimental.pallas import tpu as pltpu
from jax.sharding import PartitionSpec as P

F32 = jnp.float32
BF16 = jnp.bfloat16
GROUP = 8
ROWS = 1024
D_IN = 896
D_OUT = 4864
RANK = 8
LANES = 128
CHUNK = 256
N_CHUNK = D_OUT // CHUNK
HALF = D_OUT // 2
SIDE = D_IN // 2
SHARES = ((0, 512), (512, 512), (1024, 640), (1664, 512), (2176, 256))
LAST = len(SHARES) - 1
SLAB = 64
SLABS = SIDE // SLAB
PADDED = 4 * RANK
PAIRS = N_CHUNK // 2
MESH = pl.DeviceIdType.MESH
C0 = 0.7978845608028654
C1 = 0.044715
VMEM_MERGE = 44 * 1024 * 1024
VMEM_FACTOR = 44 * 1024 * 1024
VMEM_ERROR = 24 * 1024 * 1024


def split3(x):
    hi = x.astype(BF16)
    rest = x - hi.astype(F32)
    mid = rest.astype(BF16)
    low = (rest - mid.astype(F32)).astype(BF16)
    return hi, mid, low


def stacked(parts):
    return jnp.concatenate([p.astype(F32) for p in parts], axis=0).astype(BF16)


def gelu_grad_times(z, dy):
    x = z.astype(F32)
    sq = x * x
    s = lax.logistic(x * (2.0 * C0 + (2.0 * C0 * C1) * sq))
    r = 2.0 * C0 + (6.0 * C0 * C1) * sq
    return (s * (1.0 + ((1.0 - s) * x) * r) * dy.astype(F32)).astype(BF16)


def orthonormal_rows(p0):
    p0 = p0 / jnp.max(jnp.abs(p0), axis=1, keepdims=True)
    row = lax.broadcasted_iota(jnp.int32, (RANK, 1), 0)
    cur = p0
    for k in range(RANK):
        v = jnp.broadcast_to(cur[k:k + 1, :], cur.shape)
        inv = lax.rsqrt(jnp.sum(v * v, axis=1, keepdims=True))
        coef = jnp.sum(v * p0, axis=1, keepdims=True) * inv
        q = v * inv
        cur = jnp.where(row == k, q, cur - jnp.where(row > k, coef, 0.0) * q)
    return cur


def wide(ref, first, rows):
    return jnp.concatenate([ref[first, rows, :], ref[first + 1, rows, :]], axis=1)


def merge_kernel(a_hbm, z_hbm, dy_hbm, qt_hbm, e_hbm, m_ref, p_ref,
                 a_v, z0_v, dy0_v, z_v, dy_v, qt_v, at_ref, q3_v, g0, g1, pc0, pc1, sem_e, sem_zy, sem_a, sem_q):
    gs = (g0, g1)
    pieces = (pc0, pc1)

    def cols_of(c):
        return pl.ds(c * CHUNK if isinstance(c, int) else pl.multiple_of(c * CHUNK, CHUNK), CHUNK)

    def load_e(c):
        return pltpu.make_async_copy(e_hbm.at[:, cols_of(c)], m_ref.at[c], sem_e.at[c])

    def load_first(k):
        src, dst = ((z_hbm, z0_v), (dy_hbm, dy0_v))[k]
        return pltpu.make_async_copy(src.at[:, pl.ds(0, CHUNK)], dst, sem_zy.at[k, PAIRS])

    def load_pair(k, p):
        src, dst = ((z_hbm, z_v), (dy_hbm, dy_v))[k]
        first = (2 * p + 1) * CHUNK
        cols = pl.ds(first if isinstance(first, int) else pl.multiple_of(first, CHUNK), 2 * CHUNK)
        return pltpu.make_async_copy(src.at[:, cols], dst.at[p], sem_zy.at[k, p])

    def start_pair(p):
        load_pair(0, p).start(priority=1)
        load_pair(1, p).start(priority=1)

    def gelu_slab(c, p, half, j):
        rows = pl.ds(j * SLAB, SLAB)
        if isinstance(c, int) and c == 0:
            g = gelu_grad_times(z0_v[rows, :], dy0_v[rows, :])
        else:
            cols = pl.ds(half * CHUNK, CHUNK)
            g = gelu_grad_times(z_v[p, rows, cols], dy_v[p, rows, cols])
        for b in range(2):
            gs[c_par(c)][b, rows, :] = g[:, b * LANES:(b + 1) * LANES]

    par_box = [0]

    def c_par(c):
        return par_box[0] ^ 1

    def body_of(accs, p_acc):
        def merge_slab(c, par, q, i):
            rows = pl.ds(q * SIDE + i * SLAB, SLAB)
            m = pltpu.matmul_pop(accs[par][q][i]) * (1.0 / ROWS) + m_ref[c, rows, :]
            m_ref[c, rows, :] = m
            for t, piece in enumerate(split3(m)):
                for b in range(2):
                    pieces[par][t, b, rows, :] = piece[:, b * LANES:(b + 1) * LANES]

        def grad_step(par, q, k):
            pltpu.matmul_push_rhs(wide(gs[par], 0, pl.ds(k * CHUNK, CHUNK)), staging_register=0, mxu_index=q)
            for i in range(SLABS):
                lhs = wide(at_ref, 2 * k, pl.ds(q * SIDE + i * SLAB, SLAB))
                pltpu.matmul_acc_lhs(accs[par][q][i], lhs, load_staged_rhs=0 if i == 0 else None)

        def rank_step(q3, par, q, blk, t):
            rows = pl.ds(q * SIDE + blk * (SIDE - CHUNK), CHUNK)
            tile = jnp.concatenate([pieces[par][t, 0, rows, :], pieces[par][t, 1, rows, :]], axis=1)
            pltpu.matmul_push_rhs(tile, staging_register=1, mxu_index=q, transpose=True)
            pltpu.matmul_acc_lhs(p_acc[q][blk], q3, load_staged_rhs=1)

        def step(c, p, par, gelu, grad, merge, rank):
            par_box[0] = par
            if gelu:
                if par == 0:
                    load_pair(0, p).wait()
                    load_pair(1, p).wait()
            if merge:
                load_e(c - 1).wait()
            if rank:
                q3 = jnp.concatenate([q3_v[2 * (c - 2)], q3_v[2 * (c - 2) + 1]], axis=1)
            tiles = [(blk, t) for blk in range(2) for t in range(3)]
            mxu = []
            for k in range(4):
                if grad:
                    mxu.append(lambda q, k=k: grad_step(par, q, k))
                for n, (blk, t) in enumerate(tiles):
                    if rank and n * 4 // len(tiles) == k:
                        mxu.append(lambda q, blk=blk, t=t: rank_step(q3, par, q, blk, t))
            n_gelu = ROWS // SLAB
            if merge:
                for s in range(SLABS):
                    merge_slab(c - 1, par ^ 1, 0, s)
                    merge_slab(c - 1, par ^ 1, 1, s)
            for s in range(SLABS):
                for n, op in enumerate(mxu):
                    if n * SLABS // len(mxu) == s:
                        op(0)
                        op(1)
                if gelu:
                    for j in range(n_gelu):
                        if j * SLABS // n_gelu == s:
                            gelu_slab(c + 1, p, par, j)

        load_a = pltpu.make_async_copy(a_hbm, a_v, sem_a)
        load_q = pltpu.make_async_copy(qt_hbm, qt_v, sem_q)
        load_a.start()
        load_first(0).start()
        load_first(1).start()
        start_pair(0)
        load_q.start(priority=1)
        load_e(0).start(priority=1)
        start_pair(1)
        load_e(1).start(priority=1)
        load_e(2).start(priority=1)
        load_a.wait()
        load_first(0).wait()
        load_first(1).wait()
        par_box[0] = 1
        for b in range(ROWS // LANES):
            at_ref[b] = a_v[b * LANES:(b + 1) * LANES, :].T
            gelu_slab(0, 0, 0, 2 * b)
            gelu_slab(0, 0, 0, 2 * b + 1)
        start_pair(2)
        load_q.wait()
        qt = qt_v[...]
        q_all = stacked(split3(qt) + (jnp.zeros_like(qt),))
        for b in range(2 * N_CHUNK):
            q3_v[b] = q_all[:, b * LANES:(b + 1) * LANES]
        step(0, 0, 0, True, True, False, False)
        load_e(3).start()
        load_e(4).start()
        step(1, 0, 1, True, True, True, False)

        def pair(i, carry):
            @pl.when(i + 2 < PAIRS)
            def _():
                start_pair(i + 2)

            @pl.when(2 * i + 4 < N_CHUNK)
            def _():
                load_e(2 * i + 3).start()
                load_e(2 * i + 4).start()

            for par in range(2):
                c = 2 * i + par

                @pl.when(c + 1 < N_CHUNK)
                def _():
                    step(c, i, par, True, True, True, True)
            return carry

        lax.fori_loop(1, N_CHUNK // 2, pair, 0)
        step(N_CHUNK - 1, 0, 0, False, True, True, True)
        step(N_CHUNK, 0, 1, False, False, True, True)
        step(N_CHUNK + 1, 0, 0, False, False, False, True)
        skip = 2 * CHUNK - SIDE
        out = []
        for q in range(2):
            for blk in range(2):
                p3 = pltpu.matmul_pop(p_acc[q][blk])
                part = p3[0:8] + p3[8:16] + p3[16:24]
                out.append(part[:, skip:] if blk else part)
        p_ref[...] = jnp.concatenate(out, axis=1)

    def acc(q, rows):
        return pltpu.ACC(q)((rows, CHUNK), F32)

    pl.run_scoped(
        body_of,
        tuple(tuple(tuple(acc(q, SLAB) for _ in range(SLABS)) for q in range(2)) for _ in range(2)),
        tuple(tuple(acc(q, PADDED) for _ in range(2)) for q in range(2)))


def factor_kernel(p_in, m_in, pt_ref, qn_ref, m_ref, p_all, p3_v, pc_v, q_mine, q_part, q_pair, q_all, q_other,
                  sem_ps, sem_pr, sem_d, sem_is, sem_ir, sem_f, sem_o):
    me = lax.axis_index('data')
    core = lax.rem(me, 2)
    chip = me // 2
    mate = me + 1 - 2 * core

    barrier = pltpu.get_barrier_semaphore()
    for d in range(1, GROUP):
        pl.semaphore_signal(barrier, inc=1, device_id=(lax.rem(me + d, GROUP),), device_id_type=MESH)
    p_all[me] = p_in[...]
    pl.semaphore_wait(barrier, GROUP - 1)

    def p_copy(d):
        return pltpu.make_async_remote_copy(
            src_ref=p_in, dst_ref=p_all.at[me], send_sem=sem_ps.at[d], recv_sem=sem_pr.at[d],
            device_id=(lax.rem(me + d, GROUP),), device_id_type=MESH)

    work = [(0, 0)]
    for g in range(LAST):
        work += [(g + 1, 0), (g, 1)]
    work.append((LAST, 1))

    def split_all():
        def one(c, carry):
            for r in range(0, D_IN, SLAB):
                rows = pl.ds(r, SLAB)
                for t, piece in enumerate(split3(m_in[c, rows, :])):
                    for b in range(2):
                        pc_v[t, 2 * c + b, rows, :] = piece[:, b * LANES:(b + 1) * LANES]
            return carry

        lax.fori_loop(0, N_CHUNK, one, 0)

    def rank_block(n):
        g, mine = work[n]
        off, width = SHARES[g]
        half = core if mine else 1 - core
        first = half * (HALF // LANES) + off // LANES
        p3 = jnp.concatenate([p3_v[b] for b in range(D_IN // LANES)], axis=1)
        acc = None
        for t in range(3):
            tile = jnp.concatenate([pc_v[t, first + b] for b in range(width // LANES)], axis=1)
            part = jnp.dot(p3, tile, preferred_element_type=F32)
            acc = part if acc is None else acc + part
        dst = q_mine if mine else q_part
        dst[:, off:off + width] = acc[0:8] + acc[8:16] + acc[16:24]

    def to_mate(g):
        cols = pl.ds(*SHARES[g])
        return pltpu.make_async_remote_copy(
            src_ref=q_part.at[:, cols], dst_ref=q_pair.at[:, cols], send_sem=sem_d.at[0, g],
            recv_sem=sem_d.at[1, g], device_id=(mate,), device_id_type=MESH)

    def to_chip(g, d):
        view = q_all.at[chip, :, pl.ds(*SHARES[g])]
        return pltpu.make_async_remote_copy(
            src_ref=view, dst_ref=view, send_sem=sem_is.at[d, g], recv_sem=sem_ir.at[d, g],
            device_id=(lax.rem(me + 2 * d, GROUP),), device_id_type=MESH)

    def my_cols(g):
        off, width = SHARES[g]
        return pl.ds(pl.multiple_of(core * HALF + off, LANES), width)

    def final(g):
        view = qn_ref.at[:, my_cols(g)]
        return pltpu.make_async_remote_copy(
            src_ref=view, dst_ref=view, send_sem=sem_f.at[0, g], recv_sem=sem_f.at[1, g],
            device_id=(mate,), device_id_type=MESH)

    def to_other(d):
        return pltpu.make_async_remote_copy(
            src_ref=q_all.at[chip, :, pl.ds(*SHARES[LAST])], dst_ref=q_other.at[chip], send_sem=sem_o.at[0, d],
            recv_sem=sem_o.at[1, d], device_id=(lax.rem(mate + 2 * d, GROUP),), device_id_type=MESH)

    mate_cols = pl.ds(pl.multiple_of((1 - core) * HALF + SHARES[LAST][0], LANES), SHARES[LAST][1])

    def mean_of(parts):
        return (parts[0] + parts[1] + parts[2] + parts[3]) * (1.0 / GROUP)

    def share_chip_sum(g):
        cols = pl.ds(*SHARES[g])
        to_mate(g).wait()
        q_all[chip, :, cols] = q_mine[:, cols] + q_pair[:, cols]
        for d in (2, 1, 3):
            to_chip(g, d).start()
            if g == LAST:
                to_other(d).start()
        if g == LAST:
            to_other(0).start()

    for d in range(1, GROUP):
        p_copy(d).start()
    split_all()
    for d in range(1, GROUP):
        p_copy(d).wait()
    p_sum = p_all[0]
    for d in range(1, GROUP):
        p_sum = p_sum + p_all[d]
    p_t = orthonormal_rows(p_sum)
    pt_ref[...] = p_t
    p3 = stacked(split3(p_t) + (jnp.zeros_like(p_t),))
    for b in range(D_IN // LANES):
        p3_v[b] = p3[:, b * LANES:(b + 1) * LANES]

    for n, (g, mine) in enumerate(work):
        rank_block(n)
        if mine:
            share_chip_sum(g)
        else:
            to_mate(g).start()
    for g in range(len(SHARES)):
        cols = pl.ds(*SHARES[g])
        for d in range(1, 4):
            to_chip(g, d).wait()
        qn_ref[:, my_cols(g)] = mean_of([q_all[k, :, cols] for k in range(4)])
        if g < LAST:
            final(g).start()
    for d in range(4):
        to_other(d).wait()
    qn_ref[:, mate_cols] = mean_of([q_other[k] for k in range(4)])
    for g in range(LAST):
        final(g).wait()


def error_kernel(pt_ref, qn_ref, m_ref, e_hbm, po_hbm, qo_hbm, e_v, left_ref, right_ref, sem):
    factors = (pltpu.make_async_copy(pt_ref, po_hbm, sem.at[N_CHUNK]),
               pltpu.make_async_copy(qn_ref, qo_hbm, sem.at[N_CHUNK + 1]))
    for move in factors:
        move.start()
    ph, pm, pl_ = split3(pt_ref[...])
    qh, qm, ql = split3(qn_ref[...])
    left_ref[...] = stacked((ph, ph, ph, pm, pm, pl_)).T
    right_ref[...] = stacked((qh, qm, ql, qh, qm, qh))

    def copy(c):
        return pltpu.make_async_copy(e_v.at[c], e_hbm.at[:, pl.ds(c * CHUNK, CHUNK)], sem.at[c])

    for c in range(N_CHUNK):
        right = right_ref[:, c * CHUNK:(c + 1) * CHUNK]
        for r in range(0, D_IN, 224):
            rows = pl.ds(r, 224)
            e_v[c, rows, :] = m_ref[c, rows, :] - jnp.dot(left_ref[rows, :], right, preferred_element_type=F32)
        copy(c).start()
    for move in factors:
        move.wait()
    for c in range(N_CHUNK):
        copy(c).wait()


def per_device(act_in, pre_act, grad_out, q_init, err_mem):
    vm = pl.BlockSpec(memory_space=pltpu.VMEM)
    anyspec = pl.BlockSpec(memory_space=pl.ANY)
    merged, p_part = pl.pallas_call(
        merge_kernel,
        out_shape=(pltpu.VMEM((N_CHUNK, D_IN, CHUNK), F32), pltpu.VMEM((RANK, D_IN), F32)),
        in_specs=[anyspec, anyspec, anyspec, anyspec, anyspec],
        out_specs=(vm, vm),
        scratch_shapes=[
            pltpu.VMEM((ROWS, D_IN), BF16),
            pltpu.VMEM((ROWS, CHUNK), BF16),
            pltpu.VMEM((ROWS, CHUNK), BF16),
            pltpu.VMEM((PAIRS, ROWS, 2 * CHUNK), BF16),
            pltpu.VMEM((PAIRS, ROWS, 2 * CHUNK), BF16),
            pltpu.VMEM((RANK, D_OUT), F32),
            pltpu.VMEM((ROWS // LANES, D_IN, LANES), BF16),
            pltpu.VMEM((2 * N_CHUNK, PADDED, LANES), BF16),
            pltpu.VMEM((2, ROWS, LANES), BF16),
            pltpu.VMEM((2, ROWS, LANES), BF16),
            pltpu.VMEM((3, 2, D_IN, LANES), BF16),
            pltpu.VMEM((3, 2, D_IN, LANES), BF16),
            pltpu.SemaphoreType.DMA((N_CHUNK,)),
            pltpu.SemaphoreType.DMA((2, PAIRS + 1)),
            pltpu.SemaphoreType.DMA,
            pltpu.SemaphoreType.DMA,
        ],
        compiler_params=pltpu.CompilerParams(vmem_limit_bytes=VMEM_MERGE),
        name='merge',
    )(act_in, pre_act, grad_out, q_init.T, err_mem.reshape(D_IN, D_OUT))
    p_t, qn_t, merged = pl.pallas_call(
        factor_kernel,
        out_shape=(pltpu.VMEM((RANK, D_IN), F32), pltpu.VMEM((RANK, D_OUT), F32), pltpu.VMEM((N_CHUNK, D_IN, CHUNK), F32)),
        in_specs=[vm, vm],
        out_specs=(vm, vm, vm),
        input_output_aliases={0: 0, 1: 2},
        scratch_shapes=[
            pltpu.VMEM((GROUP, RANK, D_IN), F32),
            pltpu.VMEM((D_IN // LANES, PADDED, LANES), BF16),
            pltpu.VMEM((3, D_OUT // LANES, D_IN, LANES), BF16),
            pltpu.VMEM((RANK, HALF), F32),
            pltpu.VMEM((RANK, HALF), F32),
            pltpu.VMEM((RANK, HALF), F32),
            pltpu.VMEM((4, RANK, HALF), F32),
            pltpu.VMEM((4, RANK, SHARES[LAST][1]), F32),
            pltpu.SemaphoreType.DMA((GROUP,)),
            pltpu.SemaphoreType.DMA((GROUP,)),
            pltpu.SemaphoreType.DMA((2, len(SHARES))),
            pltpu.SemaphoreType.DMA((4, len(SHARES))),
            pltpu.SemaphoreType.DMA((4, len(SHARES))),
            pltpu.SemaphoreType.DMA((2, len(SHARES))),
            pltpu.SemaphoreType.DMA((2, 4)),
        ],
        compiler_params=pltpu.CompilerParams(
            collective_id=0, has_side_effects=True, vmem_limit_bytes=VMEM_FACTOR),
        name='factor',
    )(p_part, merged)
    err_new, p_o, qn_o = pl.pallas_call(
        error_kernel,
        out_shape=(jax.ShapeDtypeStruct((D_IN, D_OUT), F32), jax.ShapeDtypeStruct((RANK, D_IN), F32),
                   jax.ShapeDtypeStruct((RANK, D_OUT), F32)),
        in_specs=[vm, vm, vm],
        out_specs=(anyspec, anyspec, anyspec),
        scratch_shapes=[pltpu.VMEM((N_CHUNK, D_IN, CHUNK), F32), pltpu.VMEM((D_IN, 6 * RANK), BF16),
                        pltpu.VMEM((6 * RANK, D_OUT), BF16), pltpu.SemaphoreType.DMA((N_CHUNK + 2,))],
        compiler_params=pltpu.CompilerParams(vmem_limit_bytes=VMEM_ERROR),
        name='new_error',
    )(p_t, qn_t, merged)
    return p_o.T, qn_o.T, err_new[None]


def solution(mesh):
    return jax.shard_map(
        per_device, mesh=mesh,
        in_specs=(P('data', None), P('data', None), P('data', None), P(None, None), P('data', None, None)),
        out_specs=(P(None, None), P(None, None), P('data', None, None)), check_vma=False)
```
